256 devices in a mesh: ctg: 32 (over x, y, core), br: 8 (over z).
Axes of the slice: x: 4, y: 4, z: 8, core: 2. Of those that a mesh axis runs over, the one named last changes fastest.
Arguments:
- base_vm: float32 [10240], P(('ctg', 'br')), may hold values from 0.95 to 1.05
- base_va: float32 [10240], P(('ctg', 'br')), may hold values from -0.6 to 0.6
- delta_state: float32 [256, 2, 10240], P('ctg', None, 'br'), may hold values from -0.18 to 0.18
- multipliers: float32 [256, 2, 10240], P('ctg', None, 'br'), may hold values from -6 to 6
- net_inj: float32 [256, 2, 10240], P('ctg', None, 'br'), may hold values from -6 to 6
- ang_grad: float32 [256, 10240], P('ctg', 'br'), may hold values from -6 to 6
- from_bus: int32 [13312], P('br'), may hold values from 0 to 10239
- to_bus: int32 [13312], P('br'), may hold values from 0 to 10239
- status: int32 [256, 13312], P('ctg', 'br'), may hold values 0 or 1
- conduct: float32 [13312], P('br'), may hold values from 1 to 5
- suscept: float32 [13312], P('br'), may hold values from -15 to -5
- charging: float32 [13312], P('br'), may hold values from 0.1 to 0.6
- rating: float32 [13312], P('br'), may hold values from 1 to 3
- slack: float32 [256, 13312], P('ctg', 'br'), may hold values from 0.05 to 2
- zdual: float32 [256, 13312], P('ctg', 'br'), may hold values from 0.05 to 2
Outputs:
- mismatch: float32 [256, 2, 10240], P('ctg', None, 'br')
- dual_res: float32 [256, 10240], P('ctg', 'br')
- limit_res: float32 [256, 13312], P('ctg', 'br')
- ctg_norms: float32 [256, 4], P('ctg')
- total_norms: float32 [4], replicated
The draws below stay inside these ranges and needn't reach their ends.
All inputs are finite; a program needn't handle non-finite values. No bound on the sum of `status` on one device may be relied on, other than what follows from the above.
Results may differ from the reference program's by a relative error of at most 0.0003.
Values sent between devices are 32-bit elements; how exact they have to be, the bound alone decides.
No kernel may reach another device: no remote copies, remote signals or barrier semaphores. Data moves between devices by JAX's collectives and lax.ppermute only.
A program may use at most 64 MiB of HBM per device.

```python
import math
import jax
import jax.numpy as jnp
from jax import lax

NB = 10240
NL = 13312
CTG = 256


def place_ends(drawn, rng, smallest, high):
    longest = drawn.shape.index(max(drawn.shape))
    spots = []
    for shift in (0, 1):
        where = [jax.random.randint(jax.random.fold_in(rng, axis), (), 0, length) for axis, length in enumerate(drawn.shape)]
        where[longest] = (where[longest] + shift) % drawn.shape[longest]
        spots.append(tuple(where))
    return drawn.at[spots[0]].set(smallest).at[spots[1]].set(high)


def shard_levels(key, extent, shards, low, top_value):
    def one(position, shards_of):
        draws = jax.random.uniform(jax.random.fold_in(jax.random.fold_in(key, 6), position), (shards_of,), jnp.float32, low / len(shards), top_value / len(shards))
        return jnp.repeat(jnp.exp(draws), extent[position] // shards_of).reshape((-1,) + (1,) * (len(extent) - position - 1))

    loudness = one(*shards[0])
    for cut in shards[1:]:
        loudness = loudness * one(*cut)
    return loudness


def gaussian(key, extent, width, limit, split=(), dtype=jnp.bfloat16):
    array = jax.random.normal(key, extent, jnp.float32) * width
    if len(split) > 0:
        array = shard_levels(key, extent, split, -0.22, 0.18) * array
    return jnp.clip(array, min=-limit, max=limit).astype(dtype)


def setup_inputs(seed: int = 0) -> dict:
    streams_of = jax.random.split(jax.random.key(seed), 16)
    base_vm = jnp.clip(0.95 + 0.099999964 * jax.random.uniform(streams_of[0], (NB,), jnp.float32) ** shard_levels(streams_of[0], (NB,), ((0, 256),), -0.2, 0.2), 0.95, 1.05)
    base_va = gaussian(streams_of[1], (NB,), 0.1, 0.6, ((0, 256),), jnp.float32)
    delta_state = gaussian(streams_of[2], (CTG, 2, NB), 0.03, 0.18, ((0, 32), (2, 8)), jnp.float32)
    multipliers = gaussian(streams_of[3], (CTG, 2, NB), 1.0, 6.0, ((0, 32), (2, 8)), jnp.float32)
    net_inj = gaussian(streams_of[4], (CTG, 2, NB), 1.0, 6.0, ((0, 32), (2, 8)), jnp.float32)
    ang_grad = gaussian(streams_of[5], (CTG, NB), 1.0, 6.0, ((0, 32), (1, 8)), jnp.float32)
    from_bus = place_ends(jax.random.randint(streams_of[6], (NL,), 0, NB), jax.random.fold_in(streams_of[6], 1), 0, NB - 1).astype(jnp.int32)
    to_bus = place_ends(jax.random.randint(streams_of[7], (NL,), 0, NB), jax.random.fold_in(streams_of[7], 1), 0, NB - 1).astype(jnp.int32)
    status = place_ends((jax.random.randint(streams_of[8], (CTG, NL), 0, 8) < 7).astype(jnp.int32), jax.random.fold_in(streams_of[8], 1), 0, 1)
    conduct = jnp.clip(1.0 + 4.0 * jax.random.uniform(streams_of[9], (NL,), jnp.float32) ** shard_levels(streams_of[9], (NL,), ((0, 8),), -0.2, 0.2), 1.0, 5.0)
    suscept = jnp.clip(-15.0 + 10.0 * jax.random.uniform(streams_of[10], (NL,), jnp.float32) ** shard_levels(streams_of[10], (NL,), ((0, 8),), -0.2, 0.2), -15.0, -5.0)
    charging = jnp.clip(0.1 + 0.5 * jax.random.uniform(streams_of[11], (NL,), jnp.float32) ** shard_levels(streams_of[11], (NL,), ((0, 8),), -0.2, 0.2), 0.1, 0.6)
    rating = jnp.clip(1.0 + 2.0 * jax.random.uniform(streams_of[12], (NL,), jnp.float32) ** shard_levels(streams_of[12], (NL,), ((0, 8),), -0.2, 0.2), 1.0, 3.0)
    slack = jnp.clip(jnp.exp(math.log(2.0) - 3.6888794 * jax.random.uniform(streams_of[13], (CTG, NL), jnp.float32) ** shard_levels(streams_of[13], (CTG, NL), ((0, 32), (1, 8)), -0.2, 0.2)), 0.05, 2.0)
    zdual = jnp.clip(jnp.exp(math.log(2.0) - 3.6888794 * jax.random.uniform(streams_of[14], (CTG, NL), jnp.float32) ** shard_levels(streams_of[14], (CTG, NL), ((0, 32), (1, 8)), -0.2, 0.2)), 0.05, 2.0)
    return dict(base_vm=base_vm, base_va=base_va, delta_state=delta_state, multipliers=multipliers, net_inj=net_inj, ang_grad=ang_grad, from_bus=from_bus, to_bus=to_bus, status=status, conduct=conduct, suscept=suscept, charging=charging, rating=rating, slack=slack, zdual=zdual)


def branch_flows(volt_mag, volt_ang, mult_p, mult_q, from_idx, to_idx, conduct, suscept, charging, in_service):
    volt_from = volt_mag[:, from_idx]
    volt_to = volt_mag[:, to_idx]
    angle_diff = volt_ang[:, from_idx] - volt_ang[:, to_idx]
    cos_diff = jnp.cos(angle_diff)
    sin_diff = jnp.sin(angle_diff)
    volt_prod = volt_from * volt_to
    p_from = conduct * volt_from * volt_from - volt_prod * (conduct * cos_diff + suscept * sin_diff)
    q_from = -(suscept + charging) * volt_from * volt_from - volt_prod * (conduct * sin_diff - suscept * cos_diff)
    p_to = conduct * volt_to * volt_to - volt_prod * (conduct * cos_diff - suscept * sin_diff)
    q_to = -(suscept + charging) * volt_to * volt_to + volt_prod * (conduct * sin_diff + suscept * cos_diff)
    flow_dual = volt_prod * (mult_p[:, from_idx] * (conduct * sin_diff - suscept * cos_diff) - mult_q[:, from_idx] * (conduct * cos_diff + suscept * sin_diff) + mult_p[:, to_idx] * (conduct * sin_diff + suscept * cos_diff) + mult_q[:, to_idx] * (conduct * cos_diff - suscept * sin_diff))
    at_from = jnp.stack([p_from, q_from, flow_dual], 1) * in_service[:, None, :]
    at_to = jnp.stack([p_to, q_to, -flow_dual], 1) * in_service[:, None, :]
    return (at_from, at_to)

def reference(base_vm, base_va, delta_state, multipliers, net_inj, ang_grad, from_bus, to_bus, status, conduct, suscept, charging, rating, slack, zdual):
    volt_mag = base_vm[None, :] + delta_state[:, 0]
    volt_ang = base_va[None, :] + delta_state[:, 1]
    in_service = status.astype(jnp.float32)
    at_from, at_to = branch_flows(volt_mag, volt_ang, multipliers[:, 0], multipliers[:, 1], from_bus, to_bus, conduct, suscept, charging, in_service)
    scenarios = delta_state.shape[0]
    buses = delta_state.shape[2]
    summed = jnp.zeros((scenarios, 3, buses), jnp.float32)
    summed = summed.at[:, :, from_bus].add(at_from).at[:, :, to_bus].add(at_to)
    mismatch = summed[:, :2] - net_inj
    dual_res = summed[:, 2] + ang_grad
    limit_res = in_service * (at_from[:, 0] * at_from[:, 0] + at_from[:, 1] * at_from[:, 1] + slack - rating * rating)
    complement = in_service * (zdual * slack - 0.01)
    squares = jnp.stack([lax.optimization_barrier(jnp.sum(mismatch * mismatch, axis=(1, 2))), lax.optimization_barrier(jnp.sum(dual_res * dual_res, axis=1)), lax.optimization_barrier(jnp.sum(limit_res * limit_res, axis=1)), lax.optimization_barrier(jnp.sum(complement * complement, axis=1))], 1)
    ctg_norms = jnp.sqrt(squares)
    total_norms = jnp.sqrt(lax.optimization_barrier(jnp.sum(squares, axis=0)) / scenarios)
    return (mismatch, dual_res, limit_res, ctg_norms, total_norms)
```

```python
import jax
import jax.numpy as jnp
from jax import lax
from jax.experimental import pallas as pl
from jax.experimental.pallas import tpu as pltpu
from jax.sharding import PartitionSpec as P

F32 = jnp.float32
BF16 = jnp.bfloat16

DVM, DVA, MP, MQ, INJ, ANG, LIVE, ROOM, COMP, CONST, VM, VA = 0, 10, 20, 30, 40, 60, 70, 83, 96, 97, 100, 103
ROWS1 = 112
ROWS2 = 32
LIM3, SQ3 = 30, 43
ROWS3 = 48
HI = 40
HIP = 48


def pack_kernel(where, vm, va, ds, mu, inj, ang, fb, tb, g, b, h, rt, st, sl, zd, out, table, line):
    for q in range(2):
        for t in range(10):
            lanes = slice(t * 128, t * 128 + 128)
            out[:, DVM + q * 10 + t, :] = ds[:, q, lanes]
            out[:, MP + q * 10 + t, :] = mu[:, q, lanes]
            out[:, INJ + q * 10 + t, :] = inj[:, q, lanes]
    for t in range(10):
        out[:, ANG + t, :] = ang[:, t * 128 : t * 128 + 128]
    comp = jnp.zeros((8, 128), F32)
    for t in range(13):
        lanes = slice(t * 128, t * 128 + 128)
        live = st[:, lanes].astype(F32)
        slack = sl[:, lanes]
        limit = rt[t : t + 1, :]
        out[:, LIVE + t, :] = live
        out[:, ROOM + t, :] = slack - limit * limit
        gap = live * (zd[:, lanes] * slack - 0.01)
        comp = comp + gap * gap
    out[:, COMP, :] = comp
    table[0:13, :] = fb[...].astype(F32)
    table[13:26, :] = tb[...].astype(F32)
    table[26:39, :] = g[...]
    table[39:52, :] = b[...]
    table[52:65, :] = h[...]
    table[65:96, :] = jnp.zeros((31, 128), F32)
    for k in range(3):
        row = table[pl.ds(where[0] + 32 * k, 1), :]
        out[:, CONST + k, :] = jnp.broadcast_to(row, (8, 128))
    lane = lax.broadcasted_iota(jnp.int32, (8, 128), 1)
    shift = where[1]
    first = where[2]
    for ref, at in ((vm, VM), (va, VA)):
        line[...] = jnp.zeros((8, 128), F32)
        line[:, 0:40] = jnp.broadcast_to(ref[...], (8, 40))
        turned = pltpu.roll(line[...], shift, 1)
        for r in range(3):
            in_first = jnp.logical_and(first == r, lane >= shift)
            in_next = jnp.logical_and(first + 1 == r, lane < shift)
            out[:, at + r, :] = jnp.where(jnp.logical_or(in_first, in_next), turned, 0.0)
    for r in range(106, ROWS1):
        out[:, r, :] = jnp.zeros((8, 128), F32)


def spread_kernel(part, out, line):
    for k in range(3):
        line[8 * k : 8 * k + 8, :] = part[:, CONST - 96 + k, :]
    both = part[0, VM - 96 : VM - 96 + 6, :]
    for b in range(1, 8):
        both = both + part[b, VM - 96 : VM - 96 + 6, :]
    line[24:30, :] = both
    line[30:32, :] = jnp.zeros((2, 128), F32)
    whole = line[...]
    for c in range(32):
        out[c] = whole


def in_two(x):
    high = x.astype(BF16)
    low = (x - high.astype(F32)).astype(BF16)
    return high, low


def main_kernel(r1, r2, out, tab, split, onehot, got, lows, highs, vals, left, acc, numbers, sums):
    for n in range(80):
        b, t = divmod(n, 10)
        m, s = divmod(n, 5)
        for q, (at, row) in enumerate(((DVM, 24), (DVA, 27))):
            if s < 2:
                base = r2[2 * m, row + s : row + s + 1, :]
            elif s == 2:
                base = r2[2 * m, row + 2 : row + 3, :] + r2[2 * m + 1, row : row + 1, :]
            else:
                base = r2[2 * m + 1, row + s - 2 : row + s - 1, :]
            lanes = slice((n % 2) * 128, (n % 2) * 128 + 128)
            tab[q * HI + n // 2 : q * HI + n // 2 + 1, lanes] = base + r1[b, at + t : at + t + 1, :]
        for q, at in ((2, MP), (3, MQ)):
            lanes = slice((n % 2) * 128, (n % 2) * 128 + 128)
            tab[q * HI + n // 2 : q * HI + n // 2 + 1, lanes] = r1[b, at + t : at + t + 1, :]
    high, low = in_two(tab[...])
    split[:, 0:256] = high
    split[:, 256:512] = low
    acc[...] = jnp.zeros((6 * HIP, 256), F32)
    numbers[...] = lax.broadcasted_iota(jnp.int32, (256, 128), 0).astype(F32).astype(BF16)
    rows_hi = lax.broadcasted_iota(jnp.int32, (HI, 128), 0).astype(F32)

    def constant(p, t):
        k, c = divmod(p * 13 + t, 32)
        return r2[c, 8 * k : 8 * k + 8, :]

    lim_sq = jnp.zeros((8, 128), F32)
    for t in range(13):
        for e in range(2):
            index = constant(e, t)
            hi = jnp.floor(index * (1.0 / 256.0))
            highs[e] = hi
            lows[e] = index - hi * 256.0
            for r in range(8):
                row = jnp.broadcast_to(lows[e, r : r + 1, :], (256, 128)).astype(BF16)
                onehot[e, :, r * 128 : r * 128 + 128] = jnp.where(numbers[...] == row, 1.0, 0.0).astype(BF16)
            weights = onehot[e]
            picked = jnp.dot(split[...], jnp.concatenate([weights, weights], 0), preferred_element_type=F32)
            for r in range(8):
                mask = jnp.broadcast_to(highs[e, r : r + 1, :], (HI, 128)) == rows_hi
                for q in range(4):
                    part = picked[q * HI : q * HI + HI, r * 128 : r * 128 + 128]
                    got[e * 4 + q, r : r + 1, :] = jnp.sum(jnp.where(mask, part, 0.0), axis=0, keepdims=True)
        g, b, h = constant(2, t), constant(3, t), constant(4, t)
        live = r1[:, LIVE + t, :]
        room = r1[:, ROOM + t, :]
        vf, vt = got[0], got[4]
        turn = got[1] - got[5]
        cs, sn = jnp.cos(turn), jnp.sin(turn)
        u = vf * vt
        gc, bs, gs, bc = g * cs, b * sn, g * sn, b * cs
        pf = live * (g * vf * vf - u * (gc + bs))
        qf = live * (-(b + h) * vf * vf - u * (gs - bc))
        pt = live * (g * vt * vt - u * (gc - bs))
        qt = live * (-(b + h) * vt * vt + u * (gs + bc))
        fd = live * u * (got[2] * (gs - bc) - got[3] * (gc + bs) + got[6] * (gs + bc) + got[7] * (gc - bs))
        limit = live * (pf * pf + qf * qf + room)
        out[:, LIM3 + t, :] = limit
        lim_sq = lim_sq + limit * limit
        for e, three in enumerate(((pf, qf, fd), (pt, qt, -fd))):
            for k in range(3):
                vals[e * 3 + k] = three[k]
        for e in range(2):
            for r in range(8):
                mask = numbers[0:HIP, :] == jnp.broadcast_to(highs[e, r : r + 1, :], (HIP, 128)).astype(BF16)
                lanes = slice(r * 128, r * 128 + 128)
                for k in range(3):
                    high, low = in_two(jnp.broadcast_to(vals[e * 3 + k, r : r + 1, :], (HIP, 128)))
                    zero = jnp.zeros((HIP, 128), BF16)
                    left[e, k * HIP : k * HIP + HIP, lanes] = jnp.where(mask, high, zero)
                    left[e, (k + 3) * HIP : (k + 4) * HIP, lanes] = jnp.where(mask, low, zero)
            acc[...] += lax.dot_general(left[e], onehot[e], (((1,), (1,)), ((), ())), preferred_element_type=F32)

    mis_sq = jnp.zeros((8, 128), F32)
    dual_sq = jnp.zeros((8, 128), F32)
    for k in range(3):
        for half in range(2):
            sums[half, k * HIP : k * HIP + HIP, :] = (
                acc[k * HIP : k * HIP + HIP, half * 128 : half * 128 + 128]
                + acc[(k + 3) * HIP : (k + 4) * HIP, half * 128 : half * 128 + 128]
            )
    for k in range(3):
        for t in range(10):
            total = sums[t % 2, pl.ds(k * HIP + t // 2, 8, stride=5), :]
            if k < 2:
                total = total - r1[:, INJ + k * 10 + t, :]
                mis_sq = mis_sq + total * total
            else:
                total = total + r1[:, ANG + t, :]
                dual_sq = dual_sq + total * total
            out[:, k * 10 + t, :] = total
    lane = lax.broadcasted_iota(jnp.int32, (8, 128), 1)
    squares = jnp.zeros((8, 128), F32)
    for k, part in enumerate((mis_sq, dual_sq, lim_sq, r1[:, COMP, :])):
        squares = jnp.where(lane == k, jnp.sum(part), squares)
    out[:, SQ3, :] = squares
    for r in range(SQ3 + 1, ROWS3):
        out[:, r, :] = jnp.zeros((8, 128), F32)


def norms_kernel(part, norms, out):
    squares = part[:, SQ3 - 40, :]
    norms[...] = jnp.sqrt(squares)[:, 0:4]
    total = jnp.sum(squares, axis=0, keepdims=True)
    out[...] = jnp.broadcast_to(total[None], (32, 1, 128))


def unpack_kernel(r3, mismatch, dual, limit):
    for t in range(10):
        lanes = slice(t * 128, t * 128 + 128)
        for k in range(2):
            mismatch[:, k, lanes] = r3[:, k * 10 + t, :]
        dual[:, lanes] = r3[:, 20 + t, :]
    for t in range(13):
        limit[:, t * 128 : t * 128 + 128] = r3[:, LIM3 + t, :]


def total_kernel(r4, out):
    total = jnp.sum(r4[:, 0, :], axis=0, keepdims=True)
    out[...] = jnp.sqrt(total * (1.0 / 256.0))


def of(shape, dtype=F32):
    return jax.ShapeDtypeStruct(shape, dtype)


def per_device(vm, va, ds, mu, inj, ang, fb, tb, st, g, b, h, rt, sl, zd):
    c, me = lax.axis_index("ctg"), lax.axis_index("br")
    offset = (c % 2) * 64 + me * 40
    where = jnp.stack([c, offset % 128, offset // 128]).astype(jnp.int32)
    sixth = [x.reshape(13, 128) for x in (fb, tb, g, b, h, rt)]
    vmem = pl.BlockSpec(memory_space=pltpu.VMEM)
    send1 = pl.pallas_call(
        pack_kernel,
        out_shape=of((8, ROWS1, 128)),
        in_specs=[pl.BlockSpec(memory_space=pltpu.SMEM)] + [vmem] * 15,
        scratch_shapes=[pltpu.VMEM((96, 128), F32), pltpu.VMEM((8, 128), F32)],
        name="pack",
    )(where, vm.reshape(1, 40), va.reshape(1, 40), ds, mu, inj, ang, *sixth, st, sl, zd)
    r1 = lax.all_to_all(send1, "br", 0, 0, tiled=True)
    send2 = pl.pallas_call(
        spread_kernel,
        grid=(1,),
        in_specs=[pl.BlockSpec((8, 16, 128), lambda i: (0, 6, 0))],
        out_specs=pl.BlockSpec((32, ROWS2, 128), lambda i: (0, 0, 0)),
        out_shape=of((32, ROWS2, 128)),
        scratch_shapes=[pltpu.VMEM((ROWS2, 128), F32)],
        name="spread",
    )(r1)
    r2 = lax.all_to_all(send2, "ctg", 0, 0, tiled=True)
    send3 = pl.pallas_call(
        main_kernel,
        out_shape=of((8, ROWS3, 128)),
        scratch_shapes=[
            pltpu.VMEM((4 * HI, 256), F32),
            pltpu.VMEM((4 * HI, 512), BF16),
            pltpu.VMEM((2, 256, 1024), BF16),
            pltpu.VMEM((8, 8, 128), F32),
            pltpu.VMEM((2, 8, 128), F32),
            pltpu.VMEM((2, 8, 128), F32),
            pltpu.VMEM((6, 8, 128), F32),
            pltpu.VMEM((2, 6 * HIP, 1024), BF16),
            pltpu.VMEM((6 * HIP, 256), F32),
            pltpu.VMEM((256, 128), BF16),
            pltpu.VMEM((2, 3 * HIP, 128), F32),
        ],
        name="main",
    )(r1, r2)
    r3 = lax.all_to_all(send3, "br", 0, 0, tiled=True)
    norms, send4 = pl.pallas_call(
        norms_kernel,
        grid=(1,),
        in_specs=[pl.BlockSpec((8, 8, 128), lambda i: (0, 5, 0))],
        out_specs=(pl.BlockSpec((8, 4), lambda i: (0, 0)), pl.BlockSpec((32, 1, 128), lambda i: (0, 0, 0))),
        out_shape=(of((8, 4)), of((32, 1, 128))),
        name="norms",
    )(r3)
    r4 = lax.all_to_all(send4, "ctg", 0, 0, tiled=True)
    mismatch, dual, limit = pl.pallas_call(
        unpack_kernel, out_shape=(of((8, 2, 1280)), of((8, 1280)), of((8, 1664))), name="unpack"
    )(r3)
    total = pl.pallas_call(total_kernel, out_shape=of((1, 128)), name="total")(r4)
    return mismatch, dual, limit, norms, total[0, 0:4]


def solution(mesh):
    both, scen, line = P(("ctg", "br")), P("ctg", "br"), P("br")
    bus = P("ctg", None, "br")
    placed = (both, both, bus, bus, bus, scen, line, line, scen, line, line, line, line, scen, scen)
    return jax.shard_map(
        per_device,
        mesh=mesh,
        in_specs=placed,
        out_specs=(bus, scen, scen, P("ctg", None), P()),
        check_vma=False,
    )
```

```python
import jax
import jax.numpy as jnp
from jax import lax
from jax.experimental import pallas as pl
from jax.experimental.pallas import tpu as pltpu
from jax.sharding import PartitionSpec as P

F32 = jnp.float32
BF16 = jnp.bfloat16

DVM, DVA, MP, MQ, INJ, ANG, LIVE, ROOM, COMP, BASE, LAST, CONST = 0, 10, 20, 30, 40, 60, 70, 83, 96, 97, 98, 99
ROWS1 = 104
VM2, VA2 = 16, 19
ROWS2 = 24
LIM3, SQ3 = 30, 43
ROWS3 = 48
HI = 40
HIP = 48


def pack_kernel(vm, va, ds, mu, inj, ang, fb, tb, g, b, h, rt, st, sl, zd, out, table, line):
    c, me = lax.axis_index("ctg"), lax.axis_index("br")
    for q in range(2):
        for t in range(10):
            lanes = slice(t * 128, t * 128 + 128)
            out[:, DVM + q * 10 + t, :] = ds[:, q, lanes]
            out[:, MP + q * 10 + t, :] = mu[:, q, lanes]
            out[:, INJ + q * 10 + t, :] = inj[:, q, lanes]
    for t in range(10):
        out[:, ANG + t, :] = ang[:, t * 128 : t * 128 + 128]
    comp = jnp.zeros((8, 128), F32)
    for t in range(13):
        lanes = slice(t * 128, t * 128 + 128)
        live = st[:, lanes].astype(F32)
        slack = sl[:, lanes]
        limit = rt[t : t + 1, :]
        out[:, LIVE + t, :] = live
        out[:, ROOM + t, :] = slack - limit * limit
        gap = live * (zd[:, lanes] * slack - 0.01)
        comp = comp + gap * gap
    out[:, COMP, :] = comp
    table[0:13, :] = fb[...].astype(F32)
    table[13:26, :] = tb[...].astype(F32)
    table[26:39, :] = g[...]
    table[39:52, :] = b[...]
    table[52:65, :] = h[...]
    for k in range(2):
        row = table[pl.ds(c + 32 * k, 1), :]
        out[:, CONST + k, :] = jnp.broadcast_to(row, (8, 128))
    out[:, LAST, :] = jnp.broadcast_to(h[12:13, :], (8, 128))
    shift = lax.rem((c % 2) * 64 + me * 40, 128)
    line[...] = jnp.zeros((8, 128), F32)
    line[:, 0:40] = jnp.broadcast_to(vm[...], (8, 40))
    turned = pltpu.roll(line[...], shift, 1)
    line[:, 0:40] = jnp.broadcast_to(va[...], (8, 40))
    out[:, BASE, :] = turned + pltpu.roll(line[...], lax.rem(shift + 64, 128), 1)
    for r in range(CONST + 2, ROWS1):
        out[:, r, :] = jnp.zeros((8, 128), F32)


def spread_kernel(part, out, line):
    for k in range(2):
        line[8 * k : 8 * k + 8, :] = part[:, CONST - 96 + k, :]
    c = lax.axis_index("ctg")
    start = lax.broadcasted_iota(jnp.int32, (8, 128), 0) * 40 + (c % 2) * 64
    lane = lax.broadcasted_iota(jnp.int32, (8, 128), 1)
    mags = part[:, BASE - 96, :]
    angs = pltpu.roll(mags, 64, 1)
    for r in range(3):
        inside = jnp.logical_and(lane + 128 * r >= start, lane + 128 * r < start + 40)
        line[VM2 + r : VM2 + r + 1, :] = jnp.sum(jnp.where(inside, mags, 0.0), axis=0, keepdims=True)
        line[VA2 + r : VA2 + r + 1, :] = jnp.sum(jnp.where(inside, angs, 0.0), axis=0, keepdims=True)
    line[22:24, :] = jnp.zeros((2, 128), F32)
    whole = line[...]
    for i in range(32):
        out[i] = whole


def in_two(x):
    high = x.astype(BF16)
    low = (x - high.astype(F32)).astype(BF16)
    return high, low


def main_kernel(r1, r2, out, tab, split, consts, sides, acc, sums, *bufs):
    for n in range(80):
        b, t = divmod(n, 10)
        m, s = divmod(n, 5)
        lanes = slice((n % 2) * 128, (n % 2) * 128 + 128)
        for q, (at, row) in enumerate(((DVM, VM2), (DVA, VA2))):
            if s < 2:
                base = r2[2 * m, row + s : row + s + 1, :]
            elif s == 2:
                base = r2[2 * m, row + 2 : row + 3, :] + r2[2 * m + 1, row : row + 1, :]
            else:
                base = r2[2 * m + 1, row + s - 2 : row + s - 1, :]
            tab[q * HI + n // 2 : q * HI + n // 2 + 1, lanes] = base + r1[b, at + t : at + t + 1, :]
        for q, at in ((2, MP), (3, MQ)):
            tab[q * HI + n // 2 : q * HI + n // 2 + 1, lanes] = r1[b, at + t : at + t + 1, :]
    high, low = in_two(tab[...])
    for k in range(2):
        split[k] = high[:, k * 128 : k * 128 + 128]
        split[k + 2] = low[:, k * 128 : k * 128 + 128]
    acc[...] = jnp.zeros((6 * HIP, 256), F32)
    numbers = lax.broadcasted_iota(jnp.int32, (256, 128), 0).astype(F32).astype(BF16)
    for t in range(13):
        for p in range(5):
            k, c = divmod(p * 13 + t, 32)
            consts[p, t] = r2[c, 8 * k : 8 * k + 8, :] if k < 2 else r1[:, LAST, :]
        sides[0, t] = r1[:, LIVE + t, :]
        sides[1, t] = r1[:, ROOM + t, :]
    rows_hi = lax.broadcasted_iota(jnp.int32, (HI, 128), 0).astype(F32)
    one, zero = jnp.ones((256, 128), BF16), jnp.zeros((256, 128), BF16)

    def table():
        return jnp.concatenate([split[k] for k in range(4)], 1)

    def across(ref, r):
        return jnp.broadcast_to(ref[r : r + 1, :], (16, 128))

    def hot(ends, e, r):
        row = across(ends.at[2 * e + 1], r).astype(BF16)
        return jnp.where(numbers == jnp.concatenate([row] * 16, 0), one, zero)

    def gather(t, ends, got, vals):
        for e in range(2):
            index = consts[e, t]
            hi = jnp.floor(index * (1.0 / 256.0))
            ends[2 * e] = hi
            ends[2 * e + 1] = index - hi * 256.0
            for pair in range(4):
                weights = jnp.concatenate([hot(ends, e, 2 * pair), hot(ends, e, 2 * pair + 1)], 1)
                picked = jnp.dot(table(), jnp.concatenate([weights, weights], 0), preferred_element_type=F32)
                for half in range(2):
                    r = 2 * pair + half
                    mask = jnp.broadcast_to(ends[2 * e, r : r + 1, :], (HI, 128)) == rows_hi
                    for q in range(4):
                        part = picked[q * HI : q * HI + HI, half * 128 : half * 128 + 128]
                        got[e * 4 + q, r : r + 1, :] = jnp.sum(jnp.where(mask, part, 0.0), axis=0, keepdims=True)
        g, b, h = consts[2, t], consts[3, t], consts[4, t]
        live, room = sides[0, t], sides[1, t]
        vf, vt = got[0], got[4]
        turn = got[1] - got[5]
        cs, sn = jnp.cos(turn), jnp.sin(turn)
        u = vf * vt
        gc, bs, gs, bc = g * cs, b * sn, g * sn, b * cs
        pf = live * (g * vf * vf - u * (gc + bs))
        qf = live * (-(b + h) * vf * vf - u * (gs - bc))
        pt = live * (g * vt * vt - u * (gc - bs))
        qt = live * (-(b + h) * vt * vt + u * (gs + bc))
        fd = live * u * (got[2] * (gs - bc) - got[3] * (gc + bs) + got[6] * (gs + bc) + got[7] * (gc - bs))
        sides[2, t] = live * (pf * pf + qf * qf + room)
        for k, value in enumerate((pf, qf, fd, pt, qt, -fd)):
            vals[k] = value

    def scatter(ends, got, vals):
        rows, cols = [], []
        for e in range(2):
            for r in range(8):
                row = across(ends.at[2 * e], r).astype(BF16)
                mask = numbers[0:HIP, :] == jnp.concatenate([row] * 3, 0)
                highs, lows = [], []
                for k in range(3):
                    high, low = in_two(across(vals.at[e * 3 + k], r))
                    highs.append(jnp.where(mask, jnp.concatenate([high] * 3, 0), zero[0:HIP]))
                    lows.append(jnp.where(mask, jnp.concatenate([low] * 3, 0), zero[0:HIP]))
                rows.append(jnp.concatenate(highs + lows, 0))
                cols.append(hot(ends, e, r))
        rows, cols = jnp.concatenate(rows, 1), jnp.concatenate(cols, 1)
        acc[...] += lax.dot_general(rows, cols, (((1,), (1,)), ((), ())), preferred_element_type=F32)

    even, odd = bufs[:3], bufs[3:]
    gather(0, *even)

    def two(i, carry):
        gather(2 * i + 1, *odd)
        scatter(*even)
        gather(2 * i + 2, *even)
        scatter(*odd)
        return carry

    lax.fori_loop(0, 6, two, 0)
    scatter(*even)

    lim_sq = jnp.zeros((8, 128), F32)
    for t in range(13):
        limit = sides[2, t]
        out[:, LIM3 + t, :] = limit
        lim_sq = lim_sq + limit * limit
    mis_sq = jnp.zeros((8, 128), F32)
    dual_sq = jnp.zeros((8, 128), F32)
    for k in range(3):
        for half in range(2):
            lanes = slice(half * 128, half * 128 + 128)
            sums[half, k * HIP : k * HIP + HIP, :] = (
                acc[k * HIP : k * HIP + HIP, lanes] + acc[(k + 3) * HIP : (k + 4) * HIP, lanes]
            )
    for k in range(3):
        for t in range(10):
            total = sums[t % 2, pl.ds(k * HIP + t // 2, 8, stride=5), :]
            if k < 2:
                total = total - r1[:, INJ + k * 10 + t, :]
                mis_sq = mis_sq + total * total
            else:
                total = total + r1[:, ANG + t, :]
                dual_sq = dual_sq + total * total
            out[:, k * 10 + t, :] = total
    lane = lax.broadcasted_iota(jnp.int32, (8, 128), 1)
    squares = jnp.zeros((8, 128), F32)
    for k, part in enumerate((mis_sq, dual_sq, lim_sq, r1[:, COMP, :])):
        squares = jnp.where(lane == k, jnp.sum(part), squares)
    out[:, SQ3, :] = squares
    for r in range(SQ3 + 1, ROWS3):
        out[:, r, :] = jnp.zeros((8, 128), F32)


def unpack_kernel(r3, mismatch, dual, limit):
    for t in range(10):
        lanes = slice(t * 128, t * 128 + 128)
        for k in range(2):
            mismatch[:, k, lanes] = r3[:, k * 10 + t, :]
        dual[:, lanes] = r3[:, 20 + t, :]
    for t in range(13):
        limit[:, t * 128 : t * 128 + 128] = r3[:, LIM3 + t, :]


def of(shape, dtype=F32):
    return jax.ShapeDtypeStruct(shape, dtype)


def per_device(vm, va, ds, mu, inj, ang, fb, tb, st, g, b, h, rt, sl, zd):
    sixth = [x.reshape(13, 128) for x in (fb, tb, g, b, h, rt)]
    send1 = pl.pallas_call(
        pack_kernel,
        out_shape=of((8, ROWS1, 128)),
        scratch_shapes=[pltpu.VMEM((96, 128), F32), pltpu.VMEM((8, 128), F32)],
        name="pack",
    )(vm.reshape(1, 40), va.reshape(1, 40), ds, mu, inj, ang, *sixth, st, sl, zd)
    r1 = lax.all_to_all(send1, "br", 0, 0, tiled=True)
    send2 = pl.pallas_call(
        spread_kernel,
        grid=(1,),
        in_specs=[pl.BlockSpec((8, 8, 128), lambda i: (0, 12, 0))],
        out_specs=pl.BlockSpec((32, ROWS2, 128), lambda i: (0, 0, 0)),
        out_shape=of((32, ROWS2, 128)),
        scratch_shapes=[pltpu.VMEM((ROWS2, 128), F32)],
        name="spread",
    )(r1)
    r2 = lax.all_to_all(send2, "ctg", 0, 0, tiled=True)
    send3 = pl.pallas_call(
        main_kernel,
        out_shape=of((8, ROWS3, 128)),
        scratch_shapes=[
            pltpu.VMEM((4 * HI, 256), F32),
            pltpu.VMEM((4, 4 * HI, 128), BF16),
            pltpu.VMEM((5, 13, 8, 128), F32),
            pltpu.VMEM((3, 13, 8, 128), F32),
            pltpu.VMEM((6 * HIP, 256), F32),
            pltpu.VMEM((2, 3 * HIP, 128), F32),
        ]
        + [
            pltpu.VMEM((4, 8, 128), F32),
            pltpu.VMEM((8, 8, 128), F32),
            pltpu.VMEM((6, 8, 128), F32),
        ]
        * 2,
        name="main",
    )(r1, r2)
    r3 = lax.all_to_all(send3, "br", 0, 0, tiled=True)
    squares = r3[:, SQ3, :]
    send4 = jnp.broadcast_to(jnp.sum(squares, axis=0)[None, None], (32, 1, 128))
    r4 = lax.all_to_all(send4, "ctg", 0, 0, tiled=True)
    mismatch, dual, limit = pl.pallas_call(
        unpack_kernel, out_shape=(of((8, 2, 1280)), of((8, 1280)), of((8, 1664))), name="unpack"
    )(r3)
    total = jnp.sqrt(jnp.sum(r4[:, 0, 0:4], axis=0) / 256.0)
    return mismatch, dual, limit, jnp.sqrt(squares[:, 0:4]), total


def solution(mesh):
    both, scen, line = P(("ctg", "br")), P("ctg", "br"), P("br")
    bus = P("ctg", None, "br")
    placed = (both, both, bus, bus, bus, scen, line, line, scen, line, line, line, line, scen, scen)
    return jax.shard_map(
        per_device,
        mesh=mesh,
        in_specs=placed,
        out_specs=(bus, scen, scen, P("ctg", None), P()),
        check_vma=False,
    )
```

```python
import jax
import jax.numpy as jnp
from jax import lax
from jax.experimental import pallas as pl
from jax.experimental.pallas import tpu as pltpu
from jax.sharding import PartitionSpec as P

F32 = jnp.float32
BF16 = jnp.bfloat16

DVM, DVA, MP, MQ, INJ, ANG, LIVE, ROOM, COMP, BASE, LAST, CONST = 0, 10, 20, 30, 40, 60, 70, 83, 96, 97, 98, 99
ROWS1 = 104
VM2, VA2 = 16, 19
ROWS2 = 24
LIM3, SQ3 = 30, 43
ROWS3 = 48
HI = 40
HIP = 48


def pack_kernel(vm, va, ds, mu, inj, ang, fb, tb, g, b, h, rt, st, sl, zd, out, table, line):
    c, me = lax.axis_index("ctg"), lax.axis_index("br")
    for q in range(2):
        for t in range(10):
            lanes = slice(t * 128, t * 128 + 128)
            out[:, DVM + q * 10 + t, :] = ds[:, q, lanes]
            out[:, MP + q * 10 + t, :] = mu[:, q, lanes]
            out[:, INJ + q * 10 + t, :] = inj[:, q, lanes]
    for t in range(10):
        out[:, ANG + t, :] = ang[:, t * 128 : t * 128 + 128]
    comp = jnp.zeros((8, 128), F32)
    for t in range(13):
        lanes = slice(t * 128, t * 128 + 128)
        live = st[:, lanes].astype(F32)
        slack = sl[:, lanes]
        limit = rt[t : t + 1, :]
        out[:, LIVE + t, :] = live
        out[:, ROOM + t, :] = slack - limit * limit
        gap = live * (zd[:, lanes] * slack - 0.01)
        comp = comp + gap * gap
    out[:, COMP, :] = comp
    table[0:13, :] = fb[...].astype(F32)
    table[13:26, :] = tb[...].astype(F32)
    table[26:39, :] = g[...]
    table[39:52, :] = b[...]
    table[52:65, :] = h[...]
    for k in range(2):
        row = table[pl.ds(c + 32 * k, 1), :]
        out[:, CONST + k, :] = jnp.broadcast_to(row, (8, 128))
    out[:, LAST, :] = jnp.broadcast_to(h[12:13, :], (8, 128))
    shift = lax.rem((c % 2) * 64 + me * 40, 128)
    line[...] = jnp.zeros((8, 128), F32)
    line[:, 0:40] = jnp.broadcast_to(vm[...], (8, 40))
    turned = pltpu.roll(line[...], shift, 1)
    line[:, 0:40] = jnp.broadcast_to(va[...], (8, 40))
    out[:, BASE, :] = turned + pltpu.roll(line[...], lax.rem(shift + 64, 128), 1)
    for r in range(CONST + 2, ROWS1):
        out[:, r, :] = jnp.zeros((8, 128), F32)


def spread_kernel(part, out, line):
    for k in range(2):
        line[8 * k : 8 * k + 8, :] = part[:, CONST + k, :]
    c = lax.axis_index("ctg")
    start = lax.broadcasted_iota(jnp.int32, (8, 128), 0) * 40 + (c % 2) * 64
    lane = lax.broadcasted_iota(jnp.int32, (8, 128), 1)
    mags = part[:, BASE, :]
    angs = pltpu.roll(mags, 64, 1)
    for r in range(3):
        inside = jnp.logical_and(lane + 128 * r >= start, lane + 128 * r < start + 40)
        line[VM2 + r : VM2 + r + 1, :] = jnp.sum(jnp.where(inside, mags, 0.0), axis=0, keepdims=True)
        line[VA2 + r : VA2 + r + 1, :] = jnp.sum(jnp.where(inside, angs, 0.0), axis=0, keepdims=True)
    line[22:24, :] = jnp.zeros((2, 128), F32)
    whole = line[...]
    for i in range(32):
        out[i] = whole


def in_two(x):
    high = x.astype(BF16)
    low = (x - high.astype(F32)).astype(BF16)
    return high, low


def main_kernel(r1, r2, out, tab, split, consts, sides, acc, sums, *bufs):
    for n in range(80):
        b, t = divmod(n, 10)
        m, s = divmod(n, 5)
        lanes = slice((n % 2) * 128, (n % 2) * 128 + 128)
        for q, (at, row) in enumerate(((DVM, VM2), (DVA, VA2))):
            if s < 2:
                base = r2[2 * m, row + s : row + s + 1, :]
            elif s == 2:
                base = r2[2 * m, row + 2 : row + 3, :] + r2[2 * m + 1, row : row + 1, :]
            else:
                base = r2[2 * m + 1, row + s - 2 : row + s - 1, :]
            tab[q * HI + n // 2 : q * HI + n // 2 + 1, lanes] = base + r1[b, at + t : at + t + 1, :]
        for q, at in ((2, MP), (3, MQ)):
            tab[q * HI + n // 2 : q * HI + n // 2 + 1, lanes] = r1[b, at + t : at + t + 1, :]
    high, low = in_two(tab[...])
    for k in range(2):
        split[k] = high[:, k * 128 : k * 128 + 128]
        split[k + 2] = low[:, k * 128 : k * 128 + 128]
    acc[...] = jnp.zeros((6 * HIP, 256), F32)
    numbers = lax.broadcasted_iota(jnp.int32, (256, 128), 0).astype(F32).astype(BF16)
    for t in range(13):
        for p in range(5):
            k, c = divmod(p * 13 + t, 32)
            consts[p, t] = r2[c, 8 * k : 8 * k + 8, :] if k < 2 else r1[:, LAST, :]
        sides[0, t] = r1[:, LIVE + t, :]
        sides[1, t] = r1[:, ROOM + t, :]
    rows_hi = lax.broadcasted_iota(jnp.int32, (HI, 128), 0).astype(F32)
    one, zero = jnp.ones((256, 128), BF16), jnp.zeros((256, 128), BF16)

    def table():
        return jnp.concatenate([split[k] for k in range(4)], 1)

    def across(ref, r):
        return jnp.broadcast_to(ref[r : r + 1, :], (16, 128))

    def hot(ends, e, r):
        row = across(ends.at[2 * e + 1], r).astype(BF16)
        return jnp.where(numbers == jnp.concatenate([row] * 16, 0), one, zero)

    def gather(t, ends, got, vals):
        for e in range(2):
            index = consts[e, t]
            hi = jnp.floor(index * (1.0 / 256.0))
            ends[2 * e] = hi
            ends[2 * e + 1] = index - hi * 256.0
            for pair in range(4):
                weights = jnp.concatenate([hot(ends, e, 2 * pair), hot(ends, e, 2 * pair + 1)], 1)
                picked = jnp.dot(table(), jnp.concatenate([weights, weights], 0), preferred_element_type=F32)
                for half in range(2):
                    r = 2 * pair + half
                    mask = jnp.broadcast_to(ends[2 * e, r : r + 1, :], (HI, 128)) == rows_hi
                    for q in range(4):
                        part = picked[q * HI : q * HI + HI, half * 128 : half * 128 + 128]
                        got[e * 4 + q, r : r + 1, :] = jnp.sum(jnp.where(mask, part, 0.0), axis=0, keepdims=True)
        g, b, h = consts[2, t], consts[3, t], consts[4, t]
        live, room = sides[0, t], sides[1, t]
        vf, vt = got[0], got[4]
        turn = got[1] - got[5]
        cs, sn = jnp.cos(turn), jnp.sin(turn)
        u = vf * vt
        gc, bs, gs, bc = g * cs, b * sn, g * sn, b * cs
        pf = live * (g * vf * vf - u * (gc + bs))
        qf = live * (-(b + h) * vf * vf - u * (gs - bc))
        pt = live * (g * vt * vt - u * (gc - bs))
        qt = live * (-(b + h) * vt * vt + u * (gs + bc))
        fd = live * u * (got[2] * (gs - bc) - got[3] * (gc + bs) + got[6] * (gs + bc) + got[7] * (gc - bs))
        sides[2, t] = live * (pf * pf + qf * qf + room)
        for k, value in enumerate((pf, qf, fd, pt, qt, -fd)):
            vals[k] = value

    def scatter(ends, got, vals):
        rows, cols = [], []
        for e in range(2):
            for r in range(8):
                row = across(ends.at[2 * e], r).astype(BF16)
                mask = numbers[0:HIP, :] == jnp.concatenate([row] * 3, 0)
                highs, lows = [], []
                for k in range(3):
                    high, low = in_two(across(vals.at[e * 3 + k], r))
                    highs.append(jnp.where(mask, jnp.concatenate([high] * 3, 0), zero[0:HIP]))
                    lows.append(jnp.where(mask, jnp.concatenate([low] * 3, 0), zero[0:HIP]))
                rows.append(jnp.concatenate(highs + lows, 0))
                cols.append(hot(ends, e, r))
        rows, cols = jnp.concatenate(rows, 1), jnp.concatenate(cols, 1)
        acc[...] += lax.dot_general(rows, cols, (((1,), (1,)), ((), ())), preferred_element_type=F32)

    even, odd = bufs[:3], bufs[3:]
    gather(0, *even)

    def two(i, carry):
        gather(2 * i + 1, *odd)
        scatter(*even)
        gather(2 * i + 2, *even)
        scatter(*odd)
        return carry

    lax.fori_loop(0, 6, two, 0)
    scatter(*even)

    lim_sq = jnp.zeros((8, 128), F32)
    for t in range(13):
        limit = sides[2, t]
        out[:, LIM3 + t, :] = limit
        lim_sq = lim_sq + limit * limit
    mis_sq = jnp.zeros((8, 128), F32)
    dual_sq = jnp.zeros((8, 128), F32)
    for k in range(3):
        for half in range(2):
            lanes = slice(half * 128, half * 128 + 128)
            sums[half, k * HIP : k * HIP + HIP, :] = (
                acc[k * HIP : k * HIP + HIP, lanes] + acc[(k + 3) * HIP : (k + 4) * HIP, lanes]
            )
    for k in range(3):
        for t in range(10):
            total = sums[t % 2, pl.ds(k * HIP + t // 2, 8, stride=5), :]
            if k < 2:
                total = total - r1[:, INJ + k * 10 + t, :]
                mis_sq = mis_sq + total * total
            else:
                total = total + r1[:, ANG + t, :]
                dual_sq = dual_sq + total * total
            out[:, k * 10 + t, :] = total
    lane = lax.broadcasted_iota(jnp.int32, (8, 128), 1)
    squares = jnp.zeros((8, 128), F32)
    for k, part in enumerate((mis_sq, dual_sq, lim_sq, r1[:, COMP, :])):
        squares = jnp.where(lane == k, jnp.sum(part), squares)
    out[:, SQ3, :] = squares
    for r in range(SQ3 + 1, ROWS3):
        out[:, r, :] = jnp.zeros((8, 128), F32)


def unpack_kernel(r3, mismatch, dual, limit):
    for t in range(10):
        lanes = slice(t * 128, t * 128 + 128)
        for k in range(2):
            mismatch[:, k, lanes] = r3[:, k * 10 + t, :]
        dual[:, lanes] = r3[:, 20 + t, :]
    for t in range(13):
        limit[:, t * 128 : t * 128 + 128] = r3[:, LIM3 + t, :]


VM_SPEC = pl.BlockSpec(memory_space=pltpu.VMEM)


def near(x):
    return pltpu.with_memory_space_constraint(x, pltpu.VMEM)


def of(shape, dtype=F32):
    return jax.ShapeDtypeStruct(shape, dtype)


def per_device(vm, va, ds, mu, inj, ang, fb, tb, st, g, b, h, rt, sl, zd):
    sixth = [x.reshape(13, 128) for x in (fb, tb, g, b, h, rt)]
    send1 = pl.pallas_call(
        pack_kernel,
        out_shape=pltpu.VMEM((8, ROWS1, 128), F32),
        out_specs=VM_SPEC,
        scratch_shapes=[pltpu.VMEM((96, 128), F32), pltpu.VMEM((8, 128), F32)],
        name="pack",
    )(vm.reshape(1, 40), va.reshape(1, 40), ds, mu, inj, ang, *sixth, st, sl, zd)
    r1 = lax.all_to_all(send1, "br", 0, 0, tiled=True)
    send2 = pl.pallas_call(
        spread_kernel,
        in_specs=[VM_SPEC],
        out_specs=VM_SPEC,
        out_shape=pltpu.VMEM((32, ROWS2, 128), F32),
        scratch_shapes=[pltpu.VMEM((ROWS2, 128), F32)],
        name="spread",
    )(near(r1))
    r2 = lax.all_to_all(send2, "ctg", 0, 0, tiled=True)
    send3 = pl.pallas_call(
        main_kernel,
        out_shape=pltpu.VMEM((8, ROWS3, 128), F32),
        out_specs=VM_SPEC,
        in_specs=[VM_SPEC, VM_SPEC],
        scratch_shapes=[
            pltpu.VMEM((4 * HI, 256), F32),
            pltpu.VMEM((4, 4 * HI, 128), BF16),
            pltpu.VMEM((5, 13, 8, 128), F32),
            pltpu.VMEM((3, 13, 8, 128), F32),
            pltpu.VMEM((6 * HIP, 256), F32),
            pltpu.VMEM((2, 3 * HIP, 128), F32),
        ]
        + [
            pltpu.VMEM((4, 8, 128), F32),
            pltpu.VMEM((8, 8, 128), F32),
            pltpu.VMEM((6, 8, 128), F32),
        ]
        * 2,
        name="main",
    )(near(r1), near(r2))
    r3 = lax.all_to_all(send3, "br", 0, 0, tiled=True)
    squares = r3[:, SQ3, :]
    send4 = jnp.broadcast_to(jnp.sum(squares, axis=0)[None, None], (32, 1, 128))
    r4 = lax.all_to_all(send4, "ctg", 0, 0, tiled=True)
    mismatch, dual, limit = pl.pallas_call(
        unpack_kernel, out_shape=(of((8, 2, 1280)), of((8, 1280)), of((8, 1664))), name="unpack", in_specs=[VM_SPEC]
    )(near(r3))
    total = jnp.sqrt(jnp.sum(r4[:, 0, 0:4], axis=0) / 256.0)
    return mismatch, dual, limit, jnp.sqrt(squares[:, 0:4]), total


def solution(mesh):
    both, scen, line = P(("ctg", "br")), P("ctg", "br"), P("br")
    bus = P("ctg", None, "br")
    placed = (both, both, bus, bus, bus, scen, line, line, scen, line, line, line, line, scen, scen)
    return jax.shard_map(
        per_device,
        mesh=mesh,
        in_specs=placed,
        out_specs=(bus, scen, scen, P("ctg", None), P()),
        check_vma=False,
    )
```

```python
import jax
import jax.numpy as jnp
from jax import lax
from jax.experimental import pallas as pl
from jax.experimental.pallas import tpu as pltpu
from jax.sharding import PartitionSpec as P

F32 = jnp.float32
BF16 = jnp.bfloat16

DVM, DVA, MP, MQ, INJ, ANG, LIVE, ROOM, COMP, BASE, LAST, CONST = 0, 10, 20, 30, 40, 60, 70, 83, 96, 97, 98, 99
ROWS1 = 104
VM2, VA2 = 16, 19
ROWS2 = 24
LIM3, SQ3 = 30, 43
ROWS3 = 48
HI = 40


def pack_kernel(vm, va, ds, mu, inj, ang, fb, tb, g, b, h, rt, st, sl, zd, out, table, line):
    c, me = lax.axis_index("ctg"), lax.axis_index("br")
    for q in range(2):
        for t in range(10):
            lanes = slice(t * 128, t * 128 + 128)
            out[:, DVM + q * 10 + t, :] = ds[:, q, lanes]
            out[:, MP + q * 10 + t, :] = mu[:, q, lanes]
            out[:, INJ + q * 10 + t, :] = inj[:, q, lanes]
    for t in range(10):
        out[:, ANG + t, :] = ang[:, t * 128 : t * 128 + 128]
    comp = jnp.zeros((8, 128), F32)
    for t in range(13):
        lanes = slice(t * 128, t * 128 + 128)
        live = st[:, lanes].astype(F32)
        slack = sl[:, lanes]
        limit = rt[t : t + 1, :]
        out[:, LIVE + t, :] = live
        out[:, ROOM + t, :] = slack - limit * limit
        gap = live * (zd[:, lanes] * slack - 0.01)
        comp = comp + gap * gap
    out[:, COMP, :] = comp
    table[0:13, :] = fb[...].astype(F32)
    table[13:26, :] = tb[...].astype(F32)
    table[26:39, :] = g[...]
    table[39:52, :] = b[...]
    table[52:65, :] = h[...]
    for k in range(2):
        row = table[pl.ds(c + 32 * k, 1), :]
        out[:, CONST + k, :] = jnp.broadcast_to(row, (8, 128))
    out[:, LAST, :] = jnp.broadcast_to(h[12:13, :], (8, 128))
    shift = lax.rem((c % 2) * 64 + me * 40, 128)
    line[...] = jnp.zeros((8, 128), F32)
    line[:, 0:40] = jnp.broadcast_to(vm[...], (8, 40))
    turned = pltpu.roll(line[...], shift, 1)
    line[:, 0:40] = jnp.broadcast_to(va[...], (8, 40))
    out[:, BASE, :] = turned + pltpu.roll(line[...], lax.rem(shift + 64, 128), 1)
    for r in range(CONST + 2, ROWS1):
        out[:, r, :] = jnp.zeros((8, 128), F32)


def spread_kernel(part, out, line):
    for k in range(2):
        line[8 * k : 8 * k + 8, :] = part[:, CONST + k, :]
    c = lax.axis_index("ctg")
    start = lax.broadcasted_iota(jnp.int32, (8, 128), 0) * 40 + (c % 2) * 64
    lane = lax.broadcasted_iota(jnp.int32, (8, 128), 1)
    mags = part[:, BASE, :]
    angs = pltpu.roll(mags, 64, 1)
    for r in range(3):
        inside = jnp.logical_and(lane + 128 * r >= start, lane + 128 * r < start + 40)
        line[VM2 + r : VM2 + r + 1, :] = jnp.sum(jnp.where(inside, mags, 0.0), axis=0, keepdims=True)
        line[VA2 + r : VA2 + r + 1, :] = jnp.sum(jnp.where(inside, angs, 0.0), axis=0, keepdims=True)
    line[22:24, :] = jnp.zeros((2, 128), F32)
    whole = line[...]
    for i in range(32):
        out[i] = whole


def in_two(x):
    high = x.astype(BF16)
    low = (x - high.astype(F32)).astype(BF16)
    return high, low


def main_kernel(r1, r2, out, tab, split, wide, consts, sides, acc, sums, *bufs):
    for n in range(80):
        b, t = divmod(n, 10)
        m, s = divmod(n, 5)
        for q, (at, row) in enumerate(((DVM, VM2), (DVA, VA2))):
            if s < 2:
                base = r2[2 * m, row + s : row + s + 1, :]
            elif s == 2:
                base = r2[2 * m, row + 2 : row + 3, :] + r2[2 * m + 1, row : row + 1, :]
            else:
                base = r2[2 * m + 1, row + s - 2 : row + s - 1, :]
            wide[q, n] = jnp.broadcast_to(base + r1[b, at + t : at + t + 1, :], (8, 128))
        for q, at in enumerate((MP, MQ)):
            tab[n % 2, q * HI + n // 2 : q * HI + n // 2 + 1, :] = r1[b, at + t : at + t + 1, :]
    for half in range(2):
        high, low = in_two(tab[half])
        split[half, 0 : 2 * HI, :] = high
        split[half, 2 * HI : 4 * HI, :] = low
    acc[...] = jnp.zeros((6 * HI, 256), F32)
    numbers = lax.broadcasted_iota(jnp.int32, (256, 128), 0).astype(F32).astype(BF16)
    place = lax.broadcasted_iota(jnp.int32, (16, 128), 0)
    tail = (lax.rem(place, 8) + 32).astype(F32).astype(BF16)
    upper = (place < 8).astype(F32).astype(BF16) > jnp.zeros((16, 128), BF16)
    for t in range(13):
        for p in range(5):
            k, c = divmod(p * 13 + t, 32)
            consts[p, t] = r2[c, 8 * k : 8 * k + 8, :] if k < 2 else r1[:, LAST, :]
        sides[0, t] = r1[:, LIVE + t, :]
        sides[1, t] = r1[:, ROOM + t, :]
    rows_hi = lax.broadcasted_iota(jnp.int32, (HI, 128), 0).astype(F32)
    one, zero = jnp.ones((256, 128), BF16), jnp.zeros((256, 128), BF16)

    def across(ref, r):
        return jnp.broadcast_to(ref[r : r + 1, :], (16, 128))

    def hot(ends, e, r):
        row = across(ends.at[2 * e + 1], r).astype(BF16)
        return jnp.where(numbers == jnp.concatenate([row] * 16, 0), one, zero)

    def gather(t, ends, got, vals):
        for e in range(2):
            index = consts[e, t]
            hi = jnp.floor(index * (1.0 / 256.0))
            ends[2 * e] = hi
            ends[2 * e + 1] = index - hi * 256.0
            whole = index.astype(jnp.int32)
            row, lane = lax.shift_right_logical(whole, 7), jnp.bitwise_and(whole, 127)
            found = [jnp.zeros((8, 128), F32)] * 2
            for n in range(80):
                here = row == n
                for q in range(2):
                    turned = jnp.take_along_axis(wide[q, n], lane, axis=1, mode="promise_in_bounds")
                    found[q] = jnp.where(here, turned, found[q])
            for q in range(2):
                got[e * 4 + q] = found[q]
            for pair in range(4):
                weights = jnp.concatenate([hot(ends, e, 2 * pair), hot(ends, e, 2 * pair + 1)], 1)
                table = jnp.concatenate([split[0], split[1]], 1)
                picked = jnp.dot(table, weights, preferred_element_type=F32)
                for half in range(2):
                    r = 2 * pair + half
                    lanes = slice(half * 128, half * 128 + 128)
                    mask = jnp.broadcast_to(ends[2 * e, r : r + 1, :], (HI, 128)) == rows_hi
                    for q in range(2):
                        part = (
                            picked[q * HI : q * HI + HI, lanes] + picked[(q + 2) * HI : (q + 3) * HI, lanes]
                        )
                        got[e * 4 + 2 + q, r : r + 1, :] = jnp.sum(jnp.where(mask, part, 0.0), axis=0, keepdims=True)
        g, b, h = consts[2, t], consts[3, t], consts[4, t]
        live, room = sides[0, t], sides[1, t]
        vf, vt = got[0], got[4]
        turn = got[1] - got[5]
        cs, sn = jnp.cos(turn), jnp.sin(turn)
        u = vf * vt
        gc, bs, gs, bc = g * cs, b * sn, g * sn, b * cs
        pf = live * (g * vf * vf - u * (gc + bs))
        qf = live * (-(b + h) * vf * vf - u * (gs - bc))
        pt = live * (g * vt * vt - u * (gc - bs))
        qt = live * (-(b + h) * vt * vt + u * (gs + bc))
        fd = live * u * (got[2] * (gs - bc) - got[3] * (gc + bs) + got[6] * (gs + bc) + got[7] * (gc - bs))
        sides[2, t] = live * (pf * pf + qf * qf + room)
        for k, value in enumerate((pf, qf, fd, pt, qt, -fd)):
            vals[k] = value

    def scatter(ends, got, vals):
        rows, cols = [], []
        for e in range(2):
            for r in range(8):
                row = across(ends.at[2 * e], r).astype(BF16)
                masks = [numbers[0:16] == row, numbers[16:32] == row, tail == row]
                for k in range(3):
                    high, low = in_two(across(vals.at[e * 3 + k], r))
                    mixed = jnp.where(upper, high, low)
                    five = ((0, high), (1, high), (0, low), (1, low), (2, mixed))
                    rows += [jnp.where(masks[i], value, zero[0:16]) for i, value in five]
                cols.append(hot(ends, e, r))
        rows = jnp.concatenate([jnp.concatenate(rows[15 * i : 15 * i + 15], 0) for i in range(16)], 1)
        cols = jnp.concatenate(cols, 1)
        acc[...] += lax.dot_general(rows, cols, (((1,), (1,)), ((), ())), preferred_element_type=F32)

    even, odd = bufs[:3], bufs[3:]
    gather(0, *even)

    def two(i, carry):
        gather(2 * i + 1, *odd)
        scatter(*even)
        gather(2 * i + 2, *even)
        scatter(*odd)
        return carry

    lax.fori_loop(0, 6, two, 0)
    scatter(*even)

    lim_sq = jnp.zeros((8, 128), F32)
    for t in range(13):
        limit = sides[2, t]
        out[:, LIM3 + t, :] = limit
        lim_sq = lim_sq + limit * limit
    mis_sq = jnp.zeros((8, 128), F32)
    dual_sq = jnp.zeros((8, 128), F32)
    for k in range(3):
        for half in range(2):
            lanes = slice(half * 128, half * 128 + 128)
            at = 2 * HI * k
            sums[half, k * HI : k * HI + 32, :] = acc[at : at + 32, lanes] + acc[at + 32 : at + 64, lanes]
            sums[half, k * HI + 32 : k * HI + HI, :] = acc[at + 64 : at + 72, lanes] + acc[at + 72 : at + 80, lanes]
    for k in range(3):
        for t in range(10):
            total = sums[t % 2, pl.ds(k * HI + t // 2, 8, stride=5), :]
            if k < 2:
                total = total - r1[:, INJ + k * 10 + t, :]
                mis_sq = mis_sq + total * total
            else:
                total = total + r1[:, ANG + t, :]
                dual_sq = dual_sq + total * total
            out[:, k * 10 + t, :] = total
    lane = lax.broadcasted_iota(jnp.int32, (8, 128), 1)
    squares = jnp.zeros((8, 128), F32)
    for k, part in enumerate((mis_sq, dual_sq, lim_sq, r1[:, COMP, :])):
        squares = jnp.where(lane == k, jnp.sum(part), squares)
    out[:, SQ3, :] = squares
    for r in range(SQ3 + 1, ROWS3):
        out[:, r, :] = jnp.zeros((8, 128), F32)


def norms_kernel(r3, out):
    total = jnp.sum(r3[:, SQ3, :], axis=0, keepdims=True)
    out[...] = jnp.broadcast_to(total[None], (32, 1, 128))


def unpack_kernel(r3, mismatch, dual, limit):
    for t in range(10):
        lanes = slice(t * 128, t * 128 + 128)
        for k in range(2):
            mismatch[:, k, lanes] = r3[:, k * 10 + t, :]
        dual[:, lanes] = r3[:, 20 + t, :]
    for t in range(13):
        limit[:, t * 128 : t * 128 + 128] = r3[:, LIM3 + t, :]


VM_SPEC = pl.BlockSpec(memory_space=pltpu.VMEM)


def near(x):
    return pltpu.with_memory_space_constraint(x, pltpu.VMEM)


def of(shape, dtype=F32):
    return jax.ShapeDtypeStruct(shape, dtype)


def per_device(vm, va, ds, mu, inj, ang, fb, tb, st, g, b, h, rt, sl, zd):
    sixth = [x.reshape(13, 128) for x in (fb, tb, g, b, h, rt)]
    send1 = pl.pallas_call(
        pack_kernel,
        out_shape=pltpu.VMEM((8, ROWS1, 128), F32),
        out_specs=VM_SPEC,
        scratch_shapes=[pltpu.VMEM((96, 128), F32), pltpu.VMEM((8, 128), F32)],
        name="pack",
    )(vm.reshape(1, 40), va.reshape(1, 40), ds, mu, inj, ang, *sixth, st, sl, zd)
    r1 = lax.all_to_all(send1, "br", 0, 0, tiled=True)
    send2 = pl.pallas_call(
        spread_kernel,
        in_specs=[VM_SPEC],
        out_specs=VM_SPEC,
        out_shape=pltpu.VMEM((32, ROWS2, 128), F32),
        scratch_shapes=[pltpu.VMEM((ROWS2, 128), F32)],
        name="spread",
    )(near(r1))
    r2 = lax.all_to_all(send2, "ctg", 0, 0, tiled=True)
    send3 = pl.pallas_call(
        main_kernel,
        out_shape=pltpu.VMEM((8, ROWS3, 128), F32),
        out_specs=VM_SPEC,
        in_specs=[VM_SPEC, VM_SPEC],
        scratch_shapes=[
            pltpu.VMEM((2, 2 * HI, 128), F32),
            pltpu.VMEM((2, 4 * HI, 128), BF16),
            pltpu.VMEM((2, 80, 8, 128), F32),
            pltpu.VMEM((5, 13, 8, 128), F32),
            pltpu.VMEM((3, 13, 8, 128), F32),
            pltpu.VMEM((6 * HI, 256), F32),
            pltpu.VMEM((2, 3 * HI, 128), F32),
        ]
        + [
            pltpu.VMEM((4, 8, 128), F32),
            pltpu.VMEM((8, 8, 128), F32),
            pltpu.VMEM((6, 8, 128), F32),
        ]
        * 2,
        name="main",
    )(near(r1), near(r2))
    r3 = lax.all_to_all(send3, "br", 0, 0, tiled=True)
    squares = r3[:, SQ3, :]
    send4 = pl.pallas_call(
        norms_kernel,
        out_shape=pltpu.VMEM((32, 1, 128), F32),
        in_specs=[VM_SPEC],
        out_specs=VM_SPEC,
        name="norms",
    )(near(r3))
    r4 = lax.all_to_all(send4, "ctg", 0, 0, tiled=True)
    mismatch, dual, limit = pl.pallas_call(
        unpack_kernel, out_shape=(of((8, 2, 1280)), of((8, 1280)), of((8, 1664))), name="unpack", in_specs=[VM_SPEC]
    )(near(r3))
    total = jnp.sqrt(jnp.sum(r4[:, 0, 0:4], axis=0) / 256.0)
    return mismatch, dual, limit, jnp.sqrt(squares[:, 0:4]), total


def solution(mesh):
    both, scen, line = P(("ctg", "br")), P("ctg", "br"), P("br")
    bus = P("ctg", None, "br")
    placed = (both, both, bus, bus, bus, scen, line, line, scen, line, line, line, line, scen, scen)
    return jax.shard_map(
        per_device,
        mesh=mesh,
        in_specs=placed,
        out_specs=(bus, scen, scen, P("ctg", None), P()),
        check_vma=False,
    )
```

```python
import jax
import jax.numpy as jnp
from jax import lax
from jax.experimental import pallas as pl
from jax.experimental.pallas import tpu as pltpu
from jax.sharding import PartitionSpec as P

F32 = jnp.float32
BF16 = jnp.bfloat16

DVM, DVA, MP, MQ, INJ, ANG, LIVE, ROOM, COMP, BASE, LAST, CONST = 0, 10, 20, 30, 40, 60, 70, 83, 96, 97, 98, 99
ROWS1 = 104
VM2, VA2 = 16, 19
ROWS2 = 24
LIM3, SQ3 = 30, 43
ROWS3 = 48
HI = 40


def pack_kernel(vm, va, ds, mu, inj, ang, fb, tb, g, b, h, rt, st, sl, zd, out, table, line):
    c, me = lax.axis_index("ctg"), lax.axis_index("br")
    for q in range(2):
        for t in range(10):
            lanes = slice(t * 128, t * 128 + 128)
            out[:, DVM + q * 10 + t, :] = ds[:, q, lanes]
            out[:, MP + q * 10 + t, :] = mu[:, q, lanes]
            out[:, INJ + q * 10 + t, :] = inj[:, q, lanes]
    for t in range(10):
        out[:, ANG + t, :] = ang[:, t * 128 : t * 128 + 128]
    comp = jnp.zeros((8, 128), F32)
    for t in range(13):
        lanes = slice(t * 128, t * 128 + 128)
        live = st[:, lanes].astype(F32)
        slack = sl[:, lanes]
        limit = rt[t : t + 1, :]
        out[:, LIVE + t, :] = live
        out[:, ROOM + t, :] = slack - limit * limit
        gap = live * (zd[:, lanes] * slack - 0.01)
        comp = comp + gap * gap
    out[:, COMP, :] = comp
    table[0:13, :] = fb[...].astype(F32)
    table[13:26, :] = tb[...].astype(F32)
    table[26:39, :] = g[...]
    table[39:52, :] = b[...]
    table[52:65, :] = h[...]
    for k in range(2):
        row = table[pl.ds(c + 32 * k, 1), :]
        out[:, CONST + k, :] = jnp.broadcast_to(row, (8, 128))
    out[:, LAST, :] = jnp.broadcast_to(h[12:13, :], (8, 128))
    shift = lax.rem((c % 2) * 64 + me * 40, 128)
    line[...] = jnp.zeros((8, 128), F32)
    line[:, 0:40] = jnp.broadcast_to(vm[...], (8, 40))
    turned = pltpu.roll(line[...], shift, 1)
    line[:, 0:40] = jnp.broadcast_to(va[...], (8, 40))
    out[:, BASE, :] = turned + pltpu.roll(line[...], lax.rem(shift + 64, 128), 1)
    for r in range(CONST + 2, ROWS1):
        out[:, r, :] = jnp.zeros((8, 128), F32)


def spread_kernel(part, out, line):
    for k in range(2):
        line[8 * k : 8 * k + 8, :] = part[:, CONST + k, :]
    c = lax.axis_index("ctg")
    start = lax.broadcasted_iota(jnp.int32, (8, 128), 0) * 40 + (c % 2) * 64
    lane = lax.broadcasted_iota(jnp.int32, (8, 128), 1)
    mags = part[:, BASE, :]
    angs = pltpu.roll(mags, 64, 1)
    for r in range(3):
        inside = jnp.logical_and(lane + 128 * r >= start, lane + 128 * r < start + 40)
        line[VM2 + r : VM2 + r + 1, :] = jnp.sum(jnp.where(inside, mags, 0.0), axis=0, keepdims=True)
        line[VA2 + r : VA2 + r + 1, :] = jnp.sum(jnp.where(inside, angs, 0.0), axis=0, keepdims=True)
    line[22:24, :] = jnp.zeros((2, 128), F32)
    whole = line[...]
    for i in range(32):
        out[i] = whole


def in_two(x):
    high = x.astype(BF16)
    low = (x - high.astype(F32)).astype(BF16)
    return high, low


def main_kernel(r1, r2, out, tab, split, wide, consts, sides, acc, sums, *bufs):
    for n in range(80):
        b, t = divmod(n, 10)
        m, s = divmod(n, 5)
        for q, (at, row) in enumerate(((DVM, VM2), (DVA, VA2))):
            if s < 2:
                base = r2[2 * m, row + s : row + s + 1, :]
            elif s == 2:
                base = r2[2 * m, row + 2 : row + 3, :] + r2[2 * m + 1, row : row + 1, :]
            else:
                base = r2[2 * m + 1, row + s - 2 : row + s - 1, :]
            wide[q, n] = jnp.broadcast_to(base + r1[b, at + t : at + t + 1, :], (8, 128))
        for q, at in enumerate((MP, MQ)):
            tab[n % 2, q * HI + n // 2 : q * HI + n // 2 + 1, :] = r1[b, at + t : at + t + 1, :]
    for half in range(2):
        high, low = in_two(tab[half])
        split[half, 0 : 2 * HI, :] = high
        split[half, 2 * HI : 4 * HI, :] = low
    acc[...] = jnp.zeros((6 * HI, 256), F32)
    numbers = lax.broadcasted_iota(jnp.int32, (256, 128), 0).astype(F32).astype(BF16)
    place = lax.broadcasted_iota(jnp.int32, (16, 128), 0)
    tail = (lax.rem(place, 8) + 32).astype(F32).astype(BF16)
    upper = (place < 8).astype(F32).astype(BF16) > jnp.zeros((16, 128), BF16)
    for t in range(13):
        for p in range(5):
            k, c = divmod(p * 13 + t, 32)
            consts[p, t] = r2[c, 8 * k : 8 * k + 8, :] if k < 2 else r1[:, LAST, :]
        sides[0, t] = r1[:, LIVE + t, :]
        sides[1, t] = r1[:, ROOM + t, :]
    rows_hi = lax.broadcasted_iota(jnp.int32, (HI, 128), 0).astype(F32)
    one, zero = jnp.ones((256, 128), BF16), jnp.zeros((256, 128), BF16)

    def across(ref, r):
        return jnp.broadcast_to(ref[r : r + 1, :], (16, 128))

    def hot(ends, e, r):
        row = across(ends.at[2 * e + 1], r).astype(BF16)
        return jnp.where(numbers == jnp.concatenate([row] * 16, 0), one, zero)

    def gather(t, ends, got, vals):
        for e in range(2):
            index = consts[e, t]
            hi = jnp.floor(index * (1.0 / 256.0))
            ends[2 * e] = hi
            ends[2 * e + 1] = index - hi * 256.0
            whole = index.astype(jnp.int32)
            row, lane = lax.shift_right_logical(whole, 7), jnp.bitwise_and(whole, 127)
            found = [jnp.zeros((8, 128), F32)] * 2
            for n in range(80):
                here = row == n
                for q in range(2):
                    turned = jnp.take_along_axis(wide[q, n], lane, axis=1, mode="promise_in_bounds")
                    found[q] = jnp.where(here, turned, found[q])
            for q in range(2):
                got[e * 4 + q] = found[q]
            for pair in range(4):
                weights = jnp.concatenate([hot(ends, e, 2 * pair), hot(ends, e, 2 * pair + 1)], 1)
                table = jnp.concatenate([split[0], split[1]], 1)
                picked = jnp.dot(table, weights, preferred_element_type=F32)
                for half in range(2):
                    r = 2 * pair + half
                    lanes = slice(half * 128, half * 128 + 128)
                    mask = jnp.broadcast_to(ends[2 * e, r : r + 1, :], (HI, 128)) == rows_hi
                    for q in range(2):
                        part = (
                            picked[q * HI : q * HI + HI, lanes] + picked[(q + 2) * HI : (q + 3) * HI, lanes]
                        )
                        got[e * 4 + 2 + q, r : r + 1, :] = jnp.sum(jnp.where(mask, part, 0.0), axis=0, keepdims=True)
        g, b, h = consts[2, t], consts[3, t], consts[4, t]
        live, room = sides[0, t], sides[1, t]
        vf, vt = got[0], got[4]
        turn = got[1] - got[5]
        cs, sn = jnp.cos(turn), jnp.sin(turn)
        u = vf * vt
        gc, bs, gs, bc = g * cs, b * sn, g * sn, b * cs
        pf = live * (g * vf * vf - u * (gc + bs))
        qf = live * (-(b + h) * vf * vf - u * (gs - bc))
        pt = live * (g * vt * vt - u * (gc - bs))
        qt = live * (-(b + h) * vt * vt + u * (gs + bc))
        fd = live * u * (got[2] * (gs - bc) - got[3] * (gc + bs) + got[6] * (gs + bc) + got[7] * (gc - bs))
        sides[2, t] = live * (pf * pf + qf * qf + room)
        for k, value in enumerate((pf, qf, fd, pt, qt, -fd)):
            vals[k] = value

    def scatter(ends, got, vals):
        rows, cols = [], []
        for e in range(2):
            for r in range(8):
                row = across(ends.at[2 * e], r).astype(BF16)
                masks = [numbers[0:16] == row, numbers[16:32] == row, tail == row]
                for k in range(3):
                    high, low = in_two(across(vals.at[e * 3 + k], r))
                    mixed = jnp.where(upper, high, low)
                    five = ((0, high), (1, high), (0, low), (1, low), (2, mixed))
                    rows += [jnp.where(masks[i], value, zero[0:16]) for i, value in five]
                cols.append(hot(ends, e, r))
        rows = jnp.concatenate([jnp.concatenate(rows[15 * i : 15 * i + 15], 0) for i in range(16)], 1)
        cols = jnp.concatenate(cols, 1)
        acc[...] += lax.dot_general(rows, cols, (((1,), (1,)), ((), ())), preferred_element_type=F32)

    even, odd = bufs[:3], bufs[3:]
    gather(0, *even)

    def two(i, carry):
        gather(2 * i + 1, *odd)
        scatter(*even)
        gather(2 * i + 2, *even)
        scatter(*odd)
        return carry

    lax.fori_loop(0, 6, two, 0)
    scatter(*even)

    lim_sq = jnp.zeros((8, 128), F32)
    for t in range(13):
        limit = sides[2, t]
        out[:, LIM3 + t, :] = limit
        lim_sq = lim_sq + limit * limit
    mis_sq = jnp.zeros((8, 128), F32)
    dual_sq = jnp.zeros((8, 128), F32)
    for k in range(3):
        for half in range(2):
            lanes = slice(half * 128, half * 128 + 128)
            at = 2 * HI * k
            sums[half, k * HI : k * HI + 32, :] = acc[at : at + 32, lanes] + acc[at + 32 : at + 64, lanes]
            sums[half, k * HI + 32 : k * HI + HI, :] = acc[at + 64 : at + 72, lanes] + acc[at + 72 : at + 80, lanes]
    for k in range(3):
        for t in range(10):
            total = sums[t % 2, pl.ds(k * HI + t // 2, 8, stride=5), :]
            if k < 2:
                total = total - r1[:, INJ + k * 10 + t, :]
                mis_sq = mis_sq + total * total
            else:
                total = total + r1[:, ANG + t, :]
                dual_sq = dual_sq + total * total
            out[:, k * 10 + t, :] = total
    lane = lax.broadcasted_iota(jnp.int32, (8, 128), 1)
    squares = jnp.zeros((8, 128), F32)
    for k, part in enumerate((mis_sq, dual_sq, lim_sq, r1[:, COMP, :])):
        squares = jnp.where(lane == k, jnp.sum(part), squares)
    out[:, SQ3, :] = squares
    for r in range(SQ3 + 1, ROWS3):
        out[:, r, :] = jnp.zeros((8, 128), F32)


def norms_kernel(r3, out):
    total = jnp.sum(r3[:, SQ3, :], axis=0, keepdims=True)
    out[...] = jnp.broadcast_to(total[None], (32, 1, 128))


def final_kernel(r3, r4, mismatch, dual, limit, norms, total):
    for t in range(10):
        lanes = slice(t * 128, t * 128 + 128)
        for k in range(2):
            mismatch[:, k, lanes] = r3[:, k * 10 + t, :]
        dual[:, lanes] = r3[:, 20 + t, :]
    for t in range(13):
        limit[:, t * 128 : t * 128 + 128] = r3[:, LIM3 + t, :]
    norms[...] = jnp.sqrt(jnp.transpose(r3[:, SQ3, :]))[0:4]
    whole = jnp.sum(r4[:, 0, :], axis=0, keepdims=True)
    total[...] = jnp.sqrt(whole * (1.0 / 256.0))[:, 0:4]


VM_SPEC = pl.BlockSpec(memory_space=pltpu.VMEM)


def near(x):
    return pltpu.with_memory_space_constraint(x, pltpu.VMEM)


def of(shape, dtype=F32):
    return jax.ShapeDtypeStruct(shape, dtype)


def per_device(vm, va, ds, mu, inj, ang, fb, tb, st, g, b, h, rt, sl, zd):
    sixth = [x.reshape(13, 128) for x in (fb, tb, g, b, h, rt)]
    send1 = pl.pallas_call(
        pack_kernel,
        out_shape=pltpu.VMEM((8, ROWS1, 128), F32),
        out_specs=VM_SPEC,
        scratch_shapes=[pltpu.VMEM((96, 128), F32), pltpu.VMEM((8, 128), F32)],
        name="pack",
    )(vm.reshape(1, 40), va.reshape(1, 40), ds, mu, inj, ang, *sixth, st, sl, zd)
    r1 = lax.all_to_all(send1, "br", 0, 0, tiled=True)
    send2 = pl.pallas_call(
        spread_kernel,
        in_specs=[VM_SPEC],
        out_specs=VM_SPEC,
        out_shape=pltpu.VMEM((32, ROWS2, 128), F32),
        scratch_shapes=[pltpu.VMEM((ROWS2, 128), F32)],
        name="spread",
    )(near(r1))
    r2 = lax.all_to_all(send2, "ctg", 0, 0, tiled=True)
    send3 = pl.pallas_call(
        main_kernel,
        out_shape=pltpu.VMEM((8, ROWS3, 128), F32),
        out_specs=VM_SPEC,
        in_specs=[VM_SPEC, VM_SPEC],
        scratch_shapes=[
            pltpu.VMEM((2, 2 * HI, 128), F32),
            pltpu.VMEM((2, 4 * HI, 128), BF16),
            pltpu.VMEM((2, 80, 8, 128), F32),
            pltpu.VMEM((5, 13, 8, 128), F32),
            pltpu.VMEM((3, 13, 8, 128), F32),
            pltpu.VMEM((6 * HI, 256), F32),
            pltpu.VMEM((2, 3 * HI, 128), F32),
        ]
        + [
            pltpu.VMEM((4, 8, 128), F32),
            pltpu.VMEM((8, 8, 128), F32),
            pltpu.VMEM((6, 8, 128), F32),
        ]
        * 2,
        name="main",
    )(near(r1), near(r2))
    r3 = lax.all_to_all(send3, "br", 0, 0, tiled=True)
    send4 = pl.pallas_call(
        norms_kernel,
        out_shape=pltpu.VMEM((32, 1, 128), F32),
        in_specs=[VM_SPEC],
        out_specs=VM_SPEC,
        name="norms",
    )(near(r3))
    r4 = lax.all_to_all(send4, "ctg", 0, 0, tiled=True)
    mismatch, dual, limit, norms, total = pl.pallas_call(
        final_kernel,
        out_shape=(of((8, 2, 1280)), of((8, 1280)), of((8, 1664)), of((4, 8)), of((1, 4))),
        in_specs=[VM_SPEC, VM_SPEC],
        name="final",
    )(near(r3), near(r4))
    return mismatch, dual, limit, norms.T, total.reshape(4)


def solution(mesh):
    both, scen, line = P(("ctg", "br")), P("ctg", "br"), P("br")
    bus = P("ctg", None, "br")
    placed = (both, both, bus, bus, bus, scen, line, line, scen, line, line, line, line, scen, scen)
    return jax.shard_map(
        per_device,
        mesh=mesh,
        in_specs=placed,
        out_specs=(bus, scen, scen, P("ctg", None), P()),
        check_vma=False,
    )
```

```python
import jax
import jax.numpy as jnp
from jax import lax
from jax.experimental import pallas as pl
from jax.experimental.pallas import tpu as pltpu
from jax.sharding import PartitionSpec as P

F32 = jnp.float32
BF16 = jnp.bfloat16

DVM, DVA, MP, MQ, INJ, ANG, LIVE, ROOM, COMP, BASE, LAST, CONST = 0, 10, 20, 30, 40, 60, 70, 83, 96, 97, 98, 99
ROWS1 = 104
VM2, VA2 = 16, 19
ROWS2 = 24
LIM3, SQ3 = 30, 43
ROWS3 = 48
HI = 40


def pack_kernel(vm, va, ds, mu, inj, ang, fb, tb, g, b, h, rt, st, sl, zd, out, table, line):
    c, me = lax.axis_index("ctg"), lax.axis_index("br")
    for q in range(2):
        for t in range(10):
            lanes = slice(t * 128, t * 128 + 128)
            out[:, DVM + q * 10 + t, :] = ds[:, q, lanes]
            out[:, MP + q * 10 + t, :] = mu[:, q, lanes]
            out[:, INJ + q * 10 + t, :] = inj[:, q, lanes]
    for t in range(10):
        out[:, ANG + t, :] = ang[:, t * 128 : t * 128 + 128]
    comp = jnp.zeros((8, 128), F32)
    for t in range(13):
        lanes = slice(t * 128, t * 128 + 128)
        live = st[:, lanes].astype(F32)
        slack = sl[:, lanes]
        limit = rt[t : t + 1, :]
        out[:, LIVE + t, :] = live
        out[:, ROOM + t, :] = slack - limit * limit
        gap = live * (zd[:, lanes] * slack - 0.01)
        comp = comp + gap * gap
    out[:, COMP, :] = comp
    table[0:13, :] = fb[...].astype(F32)
    table[13:26, :] = tb[...].astype(F32)
    table[26:39, :] = g[...]
    table[39:52, :] = b[...]
    table[52:65, :] = h[...]
    for k in range(2):
        row = table[pl.ds(c + 32 * k, 1), :]
        out[:, CONST + k, :] = jnp.broadcast_to(row, (8, 128))
    out[:, LAST, :] = jnp.broadcast_to(h[12:13, :], (8, 128))
    shift = lax.rem((c % 2) * 64 + me * 40, 128)
    line[...] = jnp.zeros((8, 128), F32)
    line[:, 0:40] = jnp.broadcast_to(vm[...], (8, 40))
    turned = pltpu.roll(line[...], shift, 1)
    line[:, 0:40] = jnp.broadcast_to(va[...], (8, 40))
    out[:, BASE, :] = turned + pltpu.roll(line[...], lax.rem(shift + 64, 128), 1)
    for r in range(CONST + 2, ROWS1):
        out[:, r, :] = jnp.zeros((8, 128), F32)


def spread_kernel(part, out, line):
    for k in range(2):
        line[8 * k : 8 * k + 8, :] = part[:, CONST + k, :]
    c = lax.axis_index("ctg")
    start = lax.broadcasted_iota(jnp.int32, (8, 128), 0) * 40 + (c % 2) * 64
    lane = lax.broadcasted_iota(jnp.int32, (8, 128), 1)
    mags = part[:, BASE, :]
    angs = pltpu.roll(mags, 64, 1)
    for r in range(3):
        inside = jnp.logical_and(lane + 128 * r >= start, lane + 128 * r < start + 40)
        line[VM2 + r : VM2 + r + 1, :] = jnp.sum(jnp.where(inside, mags, 0.0), axis=0, keepdims=True)
        line[VA2 + r : VA2 + r + 1, :] = jnp.sum(jnp.where(inside, angs, 0.0), axis=0, keepdims=True)
    line[22:24, :] = jnp.zeros((2, 128), F32)
    whole = line[...]
    for i in range(32):
        out[i] = whole


def in_two(x):
    high = x.astype(BF16)
    low = (x - high.astype(F32)).astype(BF16)
    return high, low


def main_kernel(r1, r2, out, tab, split, wide, consts, sides, acc, sums, *bufs):
    for n in range(80):
        b, t = divmod(n, 10)
        m, s = divmod(n, 5)
        for q, (at, row) in enumerate(((DVM, VM2), (DVA, VA2))):
            if s < 2:
                base = r2[2 * m, row + s : row + s + 1, :]
            elif s == 2:
                base = r2[2 * m, row + 2 : row + 3, :] + r2[2 * m + 1, row : row + 1, :]
            else:
                base = r2[2 * m + 1, row + s - 2 : row + s - 1, :]
            wide[q, n] = jnp.broadcast_to(base + r1[b, at + t : at + t + 1, :], (8, 128))
        for q, at in enumerate((MP, MQ)):
            tab[n % 2, q * HI + n // 2 : q * HI + n // 2 + 1, :] = r1[b, at + t : at + t + 1, :]
    for half in range(2):
        high, low = in_two(tab[half])
        split[half, 0 : 2 * HI, :] = high
        split[half, 2 * HI : 4 * HI, :] = low
    acc[...] = jnp.zeros((6 * HI, 256), F32)
    numbers = lax.broadcasted_iota(jnp.int32, (256, 128), 0).astype(F32).astype(BF16)
    place = lax.broadcasted_iota(jnp.int32, (16, 128), 0)
    tail = (lax.rem(place, 8) + 32).astype(F32).astype(BF16)
    upper = (place < 8).astype(F32).astype(BF16) > jnp.zeros((16, 128), BF16)
    for t in range(13):
        for p in range(5):
            k, c = divmod(p * 13 + t, 32)
            consts[p, t] = r2[c, 8 * k : 8 * k + 8, :] if k < 2 else r1[:, LAST, :]
        sides[0, t] = r1[:, LIVE + t, :]
        sides[1, t] = r1[:, ROOM + t, :]
    rows_hi = lax.broadcasted_iota(jnp.int32, (HI, 128), 0).astype(F32)
    one, zero = jnp.ones((256, 128), BF16), jnp.zeros((256, 128), BF16)

    def across(ref, r):
        return jnp.broadcast_to(ref[r : r + 1, :], (16, 128))

    def hot(ends, e, r):
        row = across(ends.at[2 * e + 1], r).astype(BF16)
        return jnp.where(numbers == jnp.concatenate([row] * 16, 0), one, zero)

    def gather(t, ends, got, vals):
        for e in range(2):
            index = consts[e, t]
            hi = jnp.floor(index * (1.0 / 256.0))
            ends[2 * e] = hi
            ends[2 * e + 1] = index - hi * 256.0
            whole = index.astype(jnp.int32)
            row, lane = lax.shift_right_logical(whole, 7), jnp.bitwise_and(whole, 127)
            bits = [jnp.bitwise_and(row, 1 << i) != 0 for i in range(3)]
            group = lax.shift_right_logical(row, 3)
            found = [jnp.zeros((8, 128), F32)] * 2
            for n in range(10):
                here = group == n
                for q in range(2):
                    level = [
                        jnp.take_along_axis(wide[q, 8 * n + i], lane, axis=1, mode="promise_in_bounds")
                        for i in range(8)
                    ]
                    for bit in bits:
                        level = [jnp.where(bit, y, x) for x, y in zip(level[::2], level[1::2])]
                    found[q] = jnp.where(here, level[0], found[q])
            for q in range(2):
                got[e * 4 + q] = found[q]
            for pair in range(4):
                weights = jnp.concatenate([hot(ends, e, 2 * pair), hot(ends, e, 2 * pair + 1)], 1)
                table = jnp.concatenate([split[0], split[1]], 1)
                picked = jnp.dot(table, weights, preferred_element_type=F32)
                for half in range(2):
                    r = 2 * pair + half
                    lanes = slice(half * 128, half * 128 + 128)
                    wanted = jnp.broadcast_to(ends[2 * e, r : r + 1, :], (8, 128))
                    for q in range(2):
                        kept = jnp.zeros((8, 128), F32)
                        for i in range(5):
                            at = q * HI + 8 * i
                            part = picked[at : at + 8, lanes] + picked[at + 2 * HI : at + 2 * HI + 8, lanes]
                            kept = jnp.where(wanted == rows_hi[8 * i : 8 * i + 8], part, kept)
                        got[e * 4 + 2 + q, r : r + 1, :] = jnp.sum(kept, axis=0, keepdims=True)
        g, b, h = consts[2, t], consts[3, t], consts[4, t]
        live, room = sides[0, t], sides[1, t]
        vf, vt = got[0], got[4]
        turn = got[1] - got[5]
        cs, sn = jnp.cos(turn), jnp.sin(turn)
        u = vf * vt
        gc, bs, gs, bc = g * cs, b * sn, g * sn, b * cs
        pf = live * (g * vf * vf - u * (gc + bs))
        qf = live * (-(b + h) * vf * vf - u * (gs - bc))
        pt = live * (g * vt * vt - u * (gc - bs))
        qt = live * (-(b + h) * vt * vt + u * (gs + bc))
        fd = live * u * (got[2] * (gs - bc) - got[3] * (gc + bs) + got[6] * (gs + bc) + got[7] * (gc - bs))
        sides[2, t] = live * (pf * pf + qf * qf + room)
        for k, value in enumerate((pf, qf, fd, pt, qt, -fd)):
            vals[k] = value

    def scatter(ends, got, vals):
        rows, cols = [], []
        for e in range(2):
            for r in range(8):
                row = across(ends.at[2 * e], r).astype(BF16)
                masks = [numbers[0:16] == row, numbers[16:32] == row, tail == row]
                for k in range(3):
                    high, low = in_two(across(vals.at[e * 3 + k], r))
                    mixed = jnp.where(upper, high, low)
                    five = ((0, high), (1, high), (0, low), (1, low), (2, mixed))
                    rows += [jnp.where(masks[i], value, zero[0:16]) for i, value in five]
                cols.append(hot(ends, e, r))
        rows = jnp.concatenate([jnp.concatenate(rows[15 * i : 15 * i + 15], 0) for i in range(16)], 1)
        cols = jnp.concatenate(cols, 1)
        acc[...] += lax.dot_general(rows, cols, (((1,), (1,)), ((), ())), preferred_element_type=F32)

    even, odd = bufs[:3], bufs[3:]
    gather(0, *even)

    def two(i, carry):
        gather(2 * i + 1, *odd)
        scatter(*even)
        gather(2 * i + 2, *even)
        scatter(*odd)
        return carry

    lax.fori_loop(0, 6, two, 0)
    scatter(*even)

    lim_sq = jnp.zeros((8, 128), F32)
    for t in range(13):
        limit = sides[2, t]
        out[:, LIM3 + t, :] = limit
        lim_sq = lim_sq + limit * limit
    mis_sq = jnp.zeros((8, 128), F32)
    dual_sq = jnp.zeros((8, 128), F32)
    for k in range(3):
        for half in range(2):
            lanes = slice(half * 128, half * 128 + 128)
            at = 2 * HI * k
            sums[half, k * HI : k * HI + 32, :] = acc[at : at + 32, lanes] + acc[at + 32 : at + 64, lanes]
            sums[half, k * HI + 32 : k * HI + HI, :] = acc[at + 64 : at + 72, lanes] + acc[at + 72 : at + 80, lanes]
    for k in range(3):
        for t in range(10):
            total = sums[t % 2, pl.ds(k * HI + t // 2, 8, stride=5), :]
            if k < 2:
                total = total - r1[:, INJ + k * 10 + t, :]
                mis_sq = mis_sq + total * total
            else:
                total = total + r1[:, ANG + t, :]
                dual_sq = dual_sq + total * total
            out[:, k * 10 + t, :] = total
    lane = lax.broadcasted_iota(jnp.int32, (8, 128), 1)
    squares = jnp.zeros((8, 128), F32)
    for k, part in enumerate((mis_sq, dual_sq, lim_sq, r1[:, COMP, :])):
        squares = jnp.where(lane == k, jnp.sum(part), squares)
    out[:, SQ3, :] = squares
    for r in range(SQ3 + 1, ROWS3):
        out[:, r, :] = jnp.zeros((8, 128), F32)


def norms_kernel(r3, out):
    total = jnp.sum(r3[:, SQ3, :], axis=0, keepdims=True)
    out[...] = jnp.broadcast_to(total[None], (32, 1, 128))


def final_kernel(r3, r4, mismatch, dual, limit, norms, total):
    for t in range(10):
        lanes = slice(t * 128, t * 128 + 128)
        for k in range(2):
            mismatch[:, k, lanes] = r3[:, k * 10 + t, :]
        dual[:, lanes] = r3[:, 20 + t, :]
    for t in range(13):
        limit[:, t * 128 : t * 128 + 128] = r3[:, LIM3 + t, :]
    norms[...] = jnp.sqrt(jnp.transpose(r3[:, SQ3, :]))[0:4]
    whole = jnp.sum(r4[:, 0, :], axis=0, keepdims=True)
    total[...] = jnp.sqrt(whole * (1.0 / 256.0))[:, 0:4]


VM_SPEC = pl.BlockSpec(memory_space=pltpu.VMEM)


def near(x):
    return pltpu.with_memory_space_constraint(x, pltpu.VMEM)


def of(shape, dtype=F32):
    return jax.ShapeDtypeStruct(shape, dtype)


def per_device(vm, va, ds, mu, inj, ang, fb, tb, st, g, b, h, rt, sl, zd):
    sixth = [x.reshape(13, 128) for x in (fb, tb, g, b, h, rt)]
    send1 = pl.pallas_call(
        pack_kernel,
        out_shape=pltpu.VMEM((8, ROWS1, 128), F32),
        out_specs=VM_SPEC,
        scratch_shapes=[pltpu.VMEM((96, 128), F32), pltpu.VMEM((8, 128), F32)],
        name="pack",
    )(vm.reshape(1, 40), va.reshape(1, 40), ds, mu, inj, ang, *sixth, st, sl, zd)
    r1 = lax.all_to_all(send1, "br", 0, 0, tiled=True)
    send2 = pl.pallas_call(
        spread_kernel,
        in_specs=[VM_SPEC],
        out_specs=VM_SPEC,
        out_shape=pltpu.VMEM((32, ROWS2, 128), F32),
        scratch_shapes=[pltpu.VMEM((ROWS2, 128), F32)],
        name="spread",
    )(near(r1))
    r2 = lax.all_to_all(send2, "ctg", 0, 0, tiled=True)
    send3 = pl.pallas_call(
        main_kernel,
        out_shape=pltpu.VMEM((8, ROWS3, 128), F32),
        out_specs=VM_SPEC,
        in_specs=[VM_SPEC, VM_SPEC],
        scratch_shapes=[
            pltpu.VMEM((2, 2 * HI, 128), F32),
            pltpu.VMEM((2, 4 * HI, 128), BF16),
            pltpu.VMEM((2, 80, 8, 128), F32),
            pltpu.VMEM((5, 13, 8, 128), F32),
            pltpu.VMEM((3, 13, 8, 128), F32),
            pltpu.VMEM((6 * HI, 256), F32),
            pltpu.VMEM((2, 3 * HI, 128), F32),
        ]
        + [
            pltpu.VMEM((4, 8, 128), F32),
            pltpu.VMEM((8, 8, 128), F32),
            pltpu.VMEM((6, 8, 128), F32),
        ]
        * 2,
        name="main",
    )(near(r1), near(r2))
    r3 = lax.all_to_all(send3, "br", 0, 0, tiled=True)
    send4 = pl.pallas_call(
        norms_kernel,
        out_shape=pltpu.VMEM((32, 1, 128), F32),
        in_specs=[VM_SPEC],
        out_specs=VM_SPEC,
        name="norms",
    )(near(r3))
    r4 = lax.all_to_all(send4, "ctg", 0, 0, tiled=True)
    mismatch, dual, limit, norms, total = pl.pallas_call(
        final_kernel,
        out_shape=(of((8, 2, 1280)), of((8, 1280)), of((8, 1664)), of((4, 8)), of((1, 4))),
        in_specs=[VM_SPEC, VM_SPEC],
        name="final",
    )(near(r3), near(r4))
    return mismatch, dual, limit, norms.T, total.reshape(4)


def solution(mesh):
    both, scen, line = P(("ctg", "br")), P("ctg", "br"), P("br")
    bus = P("ctg", None, "br")
    placed = (both, both, bus, bus, bus, scen, line, line, scen, line, line, line, line, scen, scen)
    return jax.shard_map(
        per_device,
        mesh=mesh,
        in_specs=placed,
        out_specs=(bus, scen, scen, P("ctg", None), P()),
        check_vma=False,
    )
```

```python
import jax
import jax.numpy as jnp
from jax import lax
from jax.experimental import pallas as pl
from jax.experimental.pallas import tpu as pltpu
from jax.sharding import PartitionSpec as P

F32 = jnp.float32
BF16 = jnp.bfloat16

DVM, DVA, MP, MQ, INJ, ANG, LIVE, ROOM, COMP, BASE, LAST, CONST = 0, 10, 20, 30, 40, 60, 70, 83, 96, 97, 98, 99
ROWS1 = 104
VM2, VA2 = 16, 19
ROWS2 = 24
LIM3, SQ3 = 30, 43
ROWS3 = 48
HI = 40


def pack_kernel(vm, va, ds, mu, inj, ang, fb, tb, g, b, h, rt, st, sl, zd, out, table, line):
    c, me = lax.axis_index("ctg"), lax.axis_index("br")
    for q in range(2):
        for t in range(10):
            lanes = slice(t * 128, t * 128 + 128)
            out[:, DVM + q * 10 + t, :] = ds[:, q, lanes]
            out[:, MP + q * 10 + t, :] = mu[:, q, lanes]
            out[:, INJ + q * 10 + t, :] = inj[:, q, lanes]
    for t in range(10):
        out[:, ANG + t, :] = ang[:, t * 128 : t * 128 + 128]
    comp = jnp.zeros((8, 128), F32)
    for t in range(13):
        lanes = slice(t * 128, t * 128 + 128)
        live = st[:, lanes].astype(F32)
        slack = sl[:, lanes]
        limit = rt[t : t + 1, :]
        out[:, LIVE + t, :] = live
        out[:, ROOM + t, :] = slack - limit * limit
        gap = live * (zd[:, lanes] * slack - 0.01)
        comp = comp + gap * gap
    out[:, COMP, :] = comp
    table[0:13, :] = fb[...].astype(F32)
    table[13:26, :] = tb[...].astype(F32)
    table[26:39, :] = g[...]
    table[39:52, :] = b[...]
    table[52:65, :] = h[...]
    for k in range(2):
        row = table[pl.ds(c + 32 * k, 1), :]
        out[:, CONST + k, :] = jnp.broadcast_to(row, (8, 128))
    out[:, LAST, :] = jnp.broadcast_to(h[12:13, :], (8, 128))
    shift = lax.rem((c % 2) * 64 + me * 40, 128)
    line[...] = jnp.zeros((8, 128), F32)
    line[:, 0:40] = jnp.broadcast_to(vm[...], (8, 40))
    turned = pltpu.roll(line[...], shift, 1)
    line[:, 0:40] = jnp.broadcast_to(va[...], (8, 40))
    out[:, BASE, :] = turned + pltpu.roll(line[...], lax.rem(shift + 64, 128), 1)
    for r in range(CONST + 2, ROWS1):
        out[:, r, :] = jnp.zeros((8, 128), F32)


def spread_kernel(part, out, line):
    for k in range(2):
        line[8 * k : 8 * k + 8, :] = part[:, CONST + k, :]
    c = lax.axis_index("ctg")
    start = lax.broadcasted_iota(jnp.int32, (8, 128), 0) * 40 + (c % 2) * 64
    lane = lax.broadcasted_iota(jnp.int32, (8, 128), 1)
    mags = part[:, BASE, :]
    angs = pltpu.roll(mags, 64, 1)
    for r in range(3):
        inside = jnp.logical_and(lane + 128 * r >= start, lane + 128 * r < start + 40)
        line[VM2 + r : VM2 + r + 1, :] = jnp.sum(jnp.where(inside, mags, 0.0), axis=0, keepdims=True)
        line[VA2 + r : VA2 + r + 1, :] = jnp.sum(jnp.where(inside, angs, 0.0), axis=0, keepdims=True)
    line[22:24, :] = jnp.zeros((2, 128), F32)
    whole = line[...]
    for i in range(32):
        out[i] = whole


def in_two(x):
    high = x.astype(BF16)
    low = (x - high.astype(F32)).astype(BF16)
    return high, low


def main_kernel(r1, r2, out, tab, split, wide, consts, sides, acc, sums, *bufs):
    for n in range(80):
        b, t = divmod(n, 10)
        m, s = divmod(n, 5)
        for q, (at, row) in enumerate(((DVM, VM2), (DVA, VA2))):
            if s < 2:
                base = r2[2 * m, row + s : row + s + 1, :]
            elif s == 2:
                base = r2[2 * m, row + 2 : row + 3, :] + r2[2 * m + 1, row : row + 1, :]
            else:
                base = r2[2 * m + 1, row + s - 2 : row + s - 1, :]
            wide[q, n] = jnp.broadcast_to(base + r1[b, at + t : at + t + 1, :], (8, 128))
        for q, at in enumerate((MP, MQ)):
            tab[n % 2, q * HI + n // 2 : q * HI + n // 2 + 1, :] = r1[b, at + t : at + t + 1, :]
    for half in range(2):
        high, low = in_two(tab[half])
        split[half, 0 : 2 * HI, :] = high
        split[half, 2 * HI : 4 * HI, :] = low
    acc[...] = jnp.zeros((6 * HI, 256), F32)
    numbers = lax.broadcasted_iota(jnp.int32, (256, 128), 0).astype(F32).astype(BF16)
    place = lax.broadcasted_iota(jnp.int32, (16, 128), 0)
    tail = (lax.rem(place, 8) + 32).astype(F32).astype(BF16)
    upper = (place < 8).astype(F32).astype(BF16) > jnp.zeros((16, 128), BF16)
    for t in range(13):
        for p in range(5):
            k, c = divmod(p * 13 + t, 32)
            consts[p, t] = r2[c, 8 * k : 8 * k + 8, :] if k < 2 else r1[:, LAST, :]
        sides[0, t] = r1[:, LIVE + t, :]
        sides[1, t] = r1[:, ROOM + t, :]
    rows_hi = lax.broadcasted_iota(jnp.int32, (HI, 128), 0).astype(F32)
    one, zero = jnp.ones((256, 128), BF16), jnp.zeros((256, 128), BF16)

    def across(ref, r):
        return jnp.broadcast_to(ref[r : r + 1, :], (16, 128))

    def hot(ends, e, r):
        row = across(ends.at[2 * e + 1], r).astype(BF16)
        return jnp.where(numbers == jnp.concatenate([row] * 16, 0), one, zero)

    def gather(t, ends, got, vals):
        for e in range(2):
            index = consts[e, t]
            hi = jnp.floor(index * (1.0 / 256.0))
            ends[2 * e] = hi
            ends[2 * e + 1] = index - hi * 256.0
            whole = index.astype(jnp.int32)
            row, lane = lax.shift_right_logical(whole, 7), jnp.bitwise_and(whole, 127)
            bits = [jnp.bitwise_and(row, 1 << i) != 0 for i in range(3)]
            group = lax.shift_right_logical(row, 3)
            found = [jnp.zeros((8, 128), F32)] * 2
            for n in range(10):
                here = group == n
                for q in range(2):
                    level = [
                        jnp.take_along_axis(wide[q, 8 * n + i], lane, axis=1, mode="promise_in_bounds")
                        for i in range(8)
                    ]
                    for bit in bits:
                        level = [jnp.where(bit, y, x) for x, y in zip(level[::2], level[1::2])]
                    found[q] = jnp.where(here, level[0], found[q])
            for q in range(2):
                got[e * 4 + q] = found[q]
            for pair in range(4):
                weights = jnp.concatenate([hot(ends, e, 2 * pair), hot(ends, e, 2 * pair + 1)], 1)
                table = jnp.concatenate([split[0], split[1]], 1)
                picked = jnp.dot(table, weights, preferred_element_type=F32)
                for half in range(2):
                    r = 2 * pair + half
                    lanes = slice(half * 128, half * 128 + 128)
                    wanted = jnp.broadcast_to(ends[2 * e, r : r + 1, :], (8, 128))
                    for q in range(2):
                        kept = jnp.zeros((8, 128), F32)
                        for i in range(5):
                            at = q * HI + 8 * i
                            part = picked[at : at + 8, lanes] + picked[at + 2 * HI : at + 2 * HI + 8, lanes]
                            kept = jnp.where(wanted == rows_hi[8 * i : 8 * i + 8], part, kept)
                        got[e * 4 + 2 + q, r : r + 1, :] = jnp.sum(kept, axis=0, keepdims=True)
        g, b, h = consts[2, t], consts[3, t], consts[4, t]
        live, room = sides[0, t], sides[1, t]
        vf, vt = got[0], got[4]
        turn = got[1] - got[5]
        cs, sn = jnp.cos(turn), jnp.sin(turn)
        u = vf * vt
        gc, bs, gs, bc = g * cs, b * sn, g * sn, b * cs
        pf = live * (g * vf * vf - u * (gc + bs))
        qf = live * (-(b + h) * vf * vf - u * (gs - bc))
        pt = live * (g * vt * vt - u * (gc - bs))
        qt = live * (-(b + h) * vt * vt + u * (gs + bc))
        fd = live * u * (got[2] * (gs - bc) - got[3] * (gc + bs) + got[6] * (gs + bc) + got[7] * (gc - bs))
        sides[2, t] = live * (pf * pf + qf * qf + room)
        for k, value in enumerate((pf, qf, fd, pt, qt, -fd)):
            high = value.astype(BF16).astype(F32)
            vals[k] = high
            vals[k + 6] = value - high

    def scatter(ends, got, vals):
        rows, cols = [], []
        for e in range(2):
            for r in range(8):
                row = across(ends.at[2 * e], r).astype(BF16)
                masks = [numbers[0:16] == row, numbers[16:32] == row, tail == row]
                for k in range(3):
                    high = across(vals.at[e * 3 + k], r).astype(BF16)
                    low = across(vals.at[e * 3 + k + 6], r).astype(BF16)
                    mixed = jnp.where(upper, high, low)
                    five = ((0, high), (1, high), (0, low), (1, low), (2, mixed))
                    rows += [jnp.where(masks[i], value, zero[0:16]) for i, value in five]
                cols.append(hot(ends, e, r))
        rows = jnp.concatenate([jnp.concatenate(rows[15 * i : 15 * i + 15], 0) for i in range(16)], 1)
        cols = jnp.concatenate(cols, 1)
        acc[...] += lax.dot_general(rows, cols, (((1,), (1,)), ((), ())), preferred_element_type=F32)

    even, odd = bufs[:3], bufs[3:]
    gather(0, *even)

    def two(i, carry):
        gather(2 * i + 1, *odd)
        scatter(*even)
        gather(2 * i + 2, *even)
        scatter(*odd)
        return carry

    lax.fori_loop(0, 6, two, 0)
    scatter(*even)

    lim_sq = jnp.zeros((8, 128), F32)
    for t in range(13):
        limit = sides[2, t]
        out[:, LIM3 + t, :] = limit
        lim_sq = lim_sq + limit * limit
    mis_sq = jnp.zeros((8, 128), F32)
    dual_sq = jnp.zeros((8, 128), F32)
    for k in range(3):
        for half in range(2):
            lanes = slice(half * 128, half * 128 + 128)
            at = 2 * HI * k
            sums[half, k * HI : k * HI + 32, :] = acc[at : at + 32, lanes] + acc[at + 32 : at + 64, lanes]
            sums[half, k * HI + 32 : k * HI + HI, :] = acc[at + 64 : at + 72, lanes] + acc[at + 72 : at + 80, lanes]
    for k in range(3):
        for t in range(10):
            total = sums[t % 2, pl.ds(k * HI + t // 2, 8, stride=5), :]
            if k < 2:
                total = total - r1[:, INJ + k * 10 + t, :]
                mis_sq = mis_sq + total * total
            else:
                total = total + r1[:, ANG + t, :]
                dual_sq = dual_sq + total * total
            out[:, k * 10 + t, :] = total
    lane = lax.broadcasted_iota(jnp.int32, (8, 128), 1)
    squares = jnp.zeros((8, 128), F32)
    for k, part in enumerate((mis_sq, dual_sq, lim_sq, r1[:, COMP, :])):
        squares = jnp.where(lane == k, jnp.sum(part), squares)
    out[:, SQ3, :] = squares
    for r in range(SQ3 + 1, ROWS3):
        out[:, r, :] = jnp.zeros((8, 128), F32)


def norms_kernel(r3, out):
    total = jnp.sum(r3[:, SQ3, :], axis=0, keepdims=True)
    out[...] = jnp.broadcast_to(total[None], (32, 1, 128))


def final_kernel(r3, r4, mismatch, dual, limit, norms, total):
    for t in range(10):
        lanes = slice(t * 128, t * 128 + 128)
        for k in range(2):
            mismatch[:, k, lanes] = r3[:, k * 10 + t, :]
        dual[:, lanes] = r3[:, 20 + t, :]
    for t in range(13):
        limit[:, t * 128 : t * 128 + 128] = r3[:, LIM3 + t, :]
    norms[...] = jnp.sqrt(jnp.transpose(r3[:, SQ3, :]))[0:4]
    whole = jnp.sum(r4[:, 0, :], axis=0, keepdims=True)
    total[...] = jnp.sqrt(whole * (1.0 / 256.0))[:, 0:4]


VM_SPEC = pl.BlockSpec(memory_space=pltpu.VMEM)


def near(x):
    return pltpu.with_memory_space_constraint(x, pltpu.VMEM)


def of(shape, dtype=F32):
    return jax.ShapeDtypeStruct(shape, dtype)


def per_device(vm, va, ds, mu, inj, ang, fb, tb, st, g, b, h, rt, sl, zd):
    sixth = [x.reshape(13, 128) for x in (fb, tb, g, b, h, rt)]
    send1 = pl.pallas_call(
        pack_kernel,
        out_shape=pltpu.VMEM((8, ROWS1, 128), F32),
        out_specs=VM_SPEC,
        scratch_shapes=[pltpu.VMEM((96, 128), F32), pltpu.VMEM((8, 128), F32)],
        name="pack",
    )(vm.reshape(1, 40), va.reshape(1, 40), ds, mu, inj, ang, *sixth, st, sl, zd)
    r1 = lax.all_to_all(send1, "br", 0, 0, tiled=True)
    send2 = pl.pallas_call(
        spread_kernel,
        in_specs=[VM_SPEC],
        out_specs=VM_SPEC,
        out_shape=pltpu.VMEM((32, ROWS2, 128), F32),
        scratch_shapes=[pltpu.VMEM((ROWS2, 128), F32)],
        name="spread",
    )(near(r1))
    r2 = lax.all_to_all(send2, "ctg", 0, 0, tiled=True)
    send3 = pl.pallas_call(
        main_kernel,
        out_shape=pltpu.VMEM((8, ROWS3, 128), F32),
        out_specs=VM_SPEC,
        in_specs=[VM_SPEC, VM_SPEC],
        scratch_shapes=[
            pltpu.VMEM((2, 2 * HI, 128), F32),
            pltpu.VMEM((2, 4 * HI, 128), BF16),
            pltpu.VMEM((2, 80, 8, 128), F32),
            pltpu.VMEM((5, 13, 8, 128), F32),
            pltpu.VMEM((3, 13, 8, 128), F32),
            pltpu.VMEM((6 * HI, 256), F32),
            pltpu.VMEM((2, 3 * HI, 128), F32),
        ]
        + [
            pltpu.VMEM((4, 8, 128), F32),
            pltpu.VMEM((8, 8, 128), F32),
            pltpu.VMEM((12, 8, 128), F32),
        ]
        * 2,
        name="main",
    )(near(r1), near(r2))
    r3 = lax.all_to_all(send3, "br", 0, 0, tiled=True)
    send4 = pl.pallas_call(
        norms_kernel,
        out_shape=pltpu.VMEM((32, 1, 128), F32),
        in_specs=[VM_SPEC],
        out_specs=VM_SPEC,
        name="norms",
    )(near(r3))
    r4 = lax.all_to_all(send4, "ctg", 0, 0, tiled=True)
    mismatch, dual, limit, norms, total = pl.pallas_call(
        final_kernel,
        out_shape=(of((8, 2, 1280)), of((8, 1280)), of((8, 1664)), of((4, 8)), of((1, 4))),
        in_specs=[VM_SPEC, VM_SPEC],
        name="final",
    )(near(r3), near(r4))
    return mismatch, dual, limit, norms.T, total.reshape(4)


def solution(mesh):
    both, scen, line = P(("ctg", "br")), P("ctg", "br"), P("br")
    bus = P("ctg", None, "br")
    placed = (both, both, bus, bus, bus, scen, line, line, scen, line, line, line, line, scen, scen)
    return jax.shard_map(
        per_device,
        mesh=mesh,
        in_specs=placed,
        out_specs=(bus, scen, scen, P("ctg", None), P()),
        check_vma=False,
    )
```
